128 devices in a mesh: tp: 4 (over x), dp: 32 (over z, y, core).
Axes of the slice: x: 4, y: 4, z: 4, core: 2. Of those that a mesh axis runs over, the one named last changes fastest.
Arguments:
- hidden: bfloat16 [32, 256, 2560], P('dp')
- residual: float32 [32, 256, 2560], P('dp')
- targets: int32 [32, 256], P('dp')
- embedding: bfloat16 [50288, 2560], P('tp')
- norm_w: float32 [2560], replicated
Outputs:
- output 1: float32 [], replicated
- output 2: float32 [32, 256, 2560], P('dp')
- output 3: float32 [50288, 2560], P('tp')
- output 4: float32 [2560], replicated
All inputs are finite; a program needn't handle non-finite values.
Results may differ from the reference program's by a relative error of at most 0.001.
Values sent between devices are 32-bit elements.
A program may use at most 1 GiB of HBM per device.

```python
import jax
import jax.numpy as jnp
from jax import lax

BATCH = 32
SEQ = 256
D = 2560
VOCAB = 50288
NORM_EPS = 1e-5
HEAD_SCALE = 2.0
TOK_BLOCK = min(SEQ, 256)


def draw_targets(tgt_key):
    k_pick, k_head, k_wide = jax.random.split(tgt_key, 3)
    pick_wide = jax.random.randint(k_pick, (BATCH, SEQ), 0, 4)
    head_ids = jax.random.randint(k_head, (BATCH, SEQ), 0, VOCAB // 16)
    wide_ids = jax.random.randint(k_wide, (BATCH, SEQ), 0, VOCAB)
    targets = jnp.where(pick_wide == 0, wide_ids, head_ids)
    return targets.at[0, 0].set(VOCAB - 1).at[0, 1].set(0).astype(jnp.int32)


def setup_inputs(seed: int = 0) -> dict:
    root_key = jax.random.key(seed)
    k_hid, k_res, k_tgt, k_emb, k_norm = jax.random.split(root_key, 5)
    hidden = jax.random.normal(k_hid, (BATCH, SEQ, D), jnp.float32).astype(jnp.bfloat16)
    residual = jax.random.normal(k_res, (BATCH, SEQ, D), jnp.float32)
    targets = draw_targets(k_tgt)
    embedding = (jax.random.normal(k_emb, (VOCAB, D), jnp.float32) * (HEAD_SCALE * D ** -0.5)).astype(jnp.bfloat16)
    norm_w = 1.0 + 0.3 * jax.random.normal(k_norm, (D,), jnp.float32)
    return {'hidden': hidden, 'residual': residual, 'targets': targets, 'embedding': embedding, 'norm_w': norm_w}


def norm_apply(resid, norm_w):
    inv_rms = lax.rsqrt(jnp.mean(resid * resid, axis=-1, keepdims=True) + NORM_EPS)
    return resid * inv_rms * norm_w


def reference(hidden, residual, targets, embedding, norm_w):
    n_tok = BATCH * SEQ
    inv_n = 1.0 / n_tok
    n_blocks = n_tok // TOK_BLOCK
    resid_all = (residual + hidden.astype(jnp.float32)).reshape(n_blocks, TOK_BLOCK, D)
    tgt_all = targets.reshape(n_blocks, TOK_BLOCK)
    vocab_ids = jnp.arange(VOCAB, dtype=jnp.int32)

    def block_step(carry_acc, blk_inputs):
        grad_emb, grad_w, loss_sum = carry_acc
        resid_blk, tgt_blk = blk_inputs
        normed, norm_vjp = jax.vjp(norm_apply, resid_blk, norm_w)
        h_blk = normed.astype(jnp.bfloat16)
        logits = jnp.dot(h_blk, embedding.T, preferred_element_type=jnp.float32)
        row_max = jnp.max(logits, axis=-1, keepdims=True)
        exp_shift = jnp.exp(logits - row_max)
        sum_exp = jnp.sum(exp_shift, axis=-1, keepdims=True)
        is_target = vocab_ids[None, :] == tgt_blk[:, None]
        tgt_logit = jnp.sum(jnp.where(is_target, logits, 0.0), axis=-1)
        log_norm = row_max[:, 0] + jnp.log(sum_exp[:, 0])
        prob_rows = exp_shift / sum_exp
        dlogits = (jnp.where(is_target, prob_rows - 1.0, prob_rows) * inv_n).astype(jnp.bfloat16)
        grad_h = jnp.dot(dlogits, embedding, preferred_element_type=jnp.float32)
        grad_r, grad_wb = norm_vjp(grad_h)
        grad_emb = grad_emb + jnp.dot(dlogits.T, h_blk, preferred_element_type=jnp.float32)
        return (grad_emb, grad_w + grad_wb, loss_sum + jnp.sum(log_norm - tgt_logit)), grad_r

    init_acc = (jnp.zeros((VOCAB, D), jnp.float32), jnp.zeros((D,), jnp.float32), jnp.zeros((), jnp.float32))
    final_acc, grad_rows = lax.scan(block_step, init_acc, (resid_all, tgt_all))
    grad_emb, grad_w, loss_sum = final_acc
    return (loss_sum * inv_n, grad_rows.reshape(BATCH, SEQ, D), grad_emb, grad_w)
```

```python
import functools

import jax
import jax.numpy as jnp
from jax import lax
from jax.experimental import pallas as pl
from jax.experimental.pallas import tpu as pltpu
from jax.sharding import PartitionSpec as P


NORM_EPS = 1e-5
TOKEN_CHUNKS = (64, 32, 64, 64, 32)
STATS_CHUNK = 1
GRAD_CHUNKS = (64, 64, 64, 64, 32, 32)
ROW_BLOCK = 512
TOKEN_BLOCK = 1024
VMEM_LIMIT = 60 * 1024 * 1024
VOCAB_BLOCK = 512
LANES = 128
NT = (((1,), (1,)), ((), ()))


def logits_kernel(vocab, h_ref, emb_ref, tgt_ref, logits_ref, max_ref, sum_ref, tgt_out_ref, m_ref, s_ref, t_ref):
    step, last = pl.program_id(0), pl.num_programs(0) - 1
    rows, width = logits_ref.shape

    @pl.when(step == 0)
    def _():
        m_ref[...] = jnp.full_like(m_ref, -jnp.inf)
        s_ref[...] = jnp.zeros_like(s_ref)
        t_ref[...] = jnp.zeros_like(t_ref)

    logits = lax.dot_general(h_ref[...], emb_ref[...], NT, preferred_element_type=jnp.float32)
    logits_ref[...] = logits
    lane = lax.broadcasted_iota(jnp.int32, (rows, LANES), 1)
    parts = []
    for j in range(width // LANES):
        ids = lane + (step * width + j * LANES)
        part = jnp.where(ids < vocab, logits[:, j * LANES:(j + 1) * LANES], -jnp.inf)
        t_ref[...] += jnp.where(ids == tgt_ref[...], part, 0.0)
        parts.append(part)
    m_old = m_ref[...]
    m_new = functools.reduce(jnp.maximum, parts, m_old)
    floor = jnp.where(m_new == -jnp.inf, 0.0, m_new)
    s_new = s_ref[...] * jnp.exp(m_old - floor)
    for part in parts:
        s_new += jnp.exp(part - floor)
    m_ref[...] = m_new
    s_ref[...] = s_new

    @pl.when(step == last)
    def _():
        m_row = jnp.max(m_new, axis=1, keepdims=True)
        max_ref[...] = m_row
        sum_ref[...] = jnp.sum(s_new * jnp.exp(m_new - m_row), axis=1, keepdims=True)
        tgt_out_ref[...] = jnp.sum(t_ref[...], axis=1, keepdims=True)


def local_logits(h_act, emb, local_ids):
    rows, width = h_act.shape
    vocab = emb.shape[0]
    steps = pl.cdiv(vocab, VOCAB_BLOCK)
    column = jax.ShapeDtypeStruct((rows, 1), jnp.float32)
    return pl.pallas_call(
        functools.partial(logits_kernel, vocab),
        out_shape=(jax.ShapeDtypeStruct((rows, vocab), jnp.float32), column, column, column),
        grid=(steps,),
        in_specs=[pl.BlockSpec((rows, width), lambda i: (0, 0)),
                  pl.BlockSpec((VOCAB_BLOCK, width), lambda i: (i, 0)),
                  pl.BlockSpec((rows, 1), lambda i: (0, 0))],
        out_specs=(pl.BlockSpec((rows, VOCAB_BLOCK), lambda i: (0, i)),
                   pl.BlockSpec((rows, 1), lambda i: (0, 0)),
                   pl.BlockSpec((rows, 1), lambda i: (0, 0)),
                   pl.BlockSpec((rows, 1), lambda i: (0, 0))),
        scratch_shapes=[pltpu.VMEM((rows, LANES), jnp.float32)] * 3,
        compiler_params=pltpu.CompilerParams(vmem_limit_bytes=VMEM_LIMIT),
        cost_estimate=pl.CostEstimate(
            flops=2 * rows * vocab * width, bytes_accessed=vocab * (2 * width + 4 * rows),
            transcendentals=rows * vocab),
        name="local_logits",
    )(h_act, emb, local_ids)


def grad_h_kernel(vocab, inv_n, logits_ref, emb_ref, tgt_ref, max_ref, sum_ref, out_ref):
    step, last = pl.program_id(0), pl.num_programs(0) - 1
    rows, width = logits_ref.shape

    @pl.when(step == 0)
    def _():
        out_ref[...] = jnp.zeros_like(out_ref)

    def add(masked):
        ids = lax.broadcasted_iota(jnp.int32, (rows, width), 1) + step * width
        prob = jnp.exp(logits_ref[...] - max_ref[...]) * sum_ref[...]
        grad = prob - jnp.where(ids == tgt_ref[...], inv_n, 0.0)
        emb = emb_ref[...]
        if masked:
            grad = jnp.where(ids < vocab, grad, 0.0)
            emb_ids = lax.broadcasted_iota(jnp.int32, emb.shape, 0) + step * width
            emb = jnp.where(emb_ids < vocab, emb.astype(jnp.float32), 0.0).astype(emb.dtype)
        out_ref[...] += jnp.dot(grad.astype(jnp.bfloat16), emb, preferred_element_type=jnp.float32)

    pl.when(step < last)(lambda: add(False))
    pl.when(step == last)(lambda: add(True))


def local_grad_h(logits, emb, local_ids, row_max, scale, inv_n):
    rows, vocab = logits.shape
    width = emb.shape[1]
    return pl.pallas_call(
        functools.partial(grad_h_kernel, vocab, inv_n),
        out_shape=jax.ShapeDtypeStruct((rows, width), jnp.float32),
        grid=(pl.cdiv(vocab, VOCAB_BLOCK),),
        in_specs=[pl.BlockSpec((rows, VOCAB_BLOCK), lambda i: (0, i)),
                  pl.BlockSpec((VOCAB_BLOCK, width), lambda i: (i, 0))]
                 + [pl.BlockSpec((rows, 1), lambda i: (0, 0))] * 3,
        out_specs=pl.BlockSpec((rows, width), lambda i: (0, 0)),
        compiler_params=pltpu.CompilerParams(vmem_limit_bytes=VMEM_LIMIT),
        cost_estimate=pl.CostEstimate(
            flops=2 * rows * vocab * width, bytes_accessed=vocab * (2 * width + 4 * rows),
            transcendentals=rows * vocab),
        name="local_grad_h",
    )(logits, emb, local_ids, row_max, scale)


def cast_kernel(src_ref, dst_ref):
    dst_ref[...] = src_ref[:, : dst_ref.shape[1], :].astype(dst_ref.dtype)


def cast_tokens(gathered, n_tok):
    n_dev, n_in, width = gathered.shape
    return pl.pallas_call(
        cast_kernel,
        out_shape=jax.ShapeDtypeStruct((n_dev, n_tok, width), jnp.bfloat16),
        grid=(n_dev // 2,),
        in_specs=[pl.BlockSpec((2, n_in, width), lambda i: (i, 0, 0))],
        out_specs=pl.BlockSpec((2, n_tok, width), lambda i: (i, 0, 0)),
        cost_estimate=pl.CostEstimate(
            flops=gathered.size * 40, bytes_accessed=gathered.size * 6, transcendentals=0),
        name="cast_tokens",
    )(gathered).reshape(n_dev * n_tok, width)


def grad_rows_kernel(has_prev, inv_n, emb_ref, rid_ref, h_ref, stats_ref, *refs):
    acc_ref = refs[-1]

    @pl.when(pl.program_id(1) == 0)
    def _():
        if has_prev:
            acc_ref[...] = refs[0][...]
        else:
            acc_ref[...] = jnp.zeros_like(acc_ref)

    h_blk = h_ref[...]
    logits = lax.dot_general(emb_ref[...], h_blk, NT, preferred_element_type=jnp.float32)
    prob = jnp.exp(logits - stats_ref[0:1, :]) * stats_ref[1:2, :]
    grad = prob - jnp.where(rid_ref[...] == stats_ref[2:3, :], inv_n, 0.0)
    acc_ref[...] += jnp.dot(grad.astype(jnp.bfloat16), h_blk, preferred_element_type=jnp.float32)


def grad_rows(emb, rid, h_chunk, stats, prev, inv_n, n_out, first_block, n_blocks, row_block):
    width = emb.shape[1]
    n_tok = h_chunk.shape[0]
    tok_block = min(TOKEN_BLOCK, n_tok)
    in_specs = [
        pl.BlockSpec((row_block, width), lambda i, t: (i + first_block, 0)),
        pl.BlockSpec((row_block, 1), lambda i, t: (i + first_block, 0)),
        pl.BlockSpec((tok_block, width), lambda i, t: (t, 0)),
        pl.BlockSpec((8, tok_block), lambda i, t: (0, t)),
    ]
    args = [emb, rid, h_chunk, stats]
    aliases = {}
    if prev is not None:
        in_specs.append(pl.BlockSpec((row_block, width), lambda i, t: (i + first_block, 0)))
        args.append(prev)
        aliases = {4: 0}
    rows = n_blocks * row_block
    return pl.pallas_call(
        functools.partial(grad_rows_kernel, prev is not None, inv_n),
        out_shape=jax.ShapeDtypeStruct((n_out, width), jnp.float32),
        grid=(n_blocks, n_tok // tok_block),
        in_specs=in_specs,
        out_specs=pl.BlockSpec((row_block, width), lambda i, t: (i + first_block, 0)),
        input_output_aliases=aliases,
        compiler_params=pltpu.CompilerParams(vmem_limit_bytes=VMEM_LIMIT),
        cost_estimate=pl.CostEstimate(
            flops=4 * rows * n_tok * width,
            bytes_accessed=rows * width * 10 + n_blocks * n_tok * width * 2,
            transcendentals=rows * n_tok),
        name="grad_rows",
    )(*args)


def place_kernel(src_ref, prev_ref, dst_ref):
    del prev_ref
    dst_ref[...] = src_ref[0, : dst_ref.shape[0], :]


def place_rows(gathered, n_rows, out, first_row):
    n_dev, n_in, width = gathered.shape
    first_block = first_row // n_rows
    return pl.pallas_call(
        place_kernel,
        out_shape=jax.ShapeDtypeStruct(out.shape, out.dtype),
        grid=(n_dev,),
        in_specs=[pl.BlockSpec((1, n_in, width), lambda i: (i, 0, 0)),
                  pl.BlockSpec(memory_space=pl.ANY)],
        out_specs=pl.BlockSpec((n_rows, width), lambda i: (i + first_block, 0)),
        input_output_aliases={1: 0},
        cost_estimate=pl.CostEstimate(
            flops=gathered.size * 80, bytes_accessed=gathered.size * 8, transcendentals=0),
        name="place_rows",
    )(gathered, out)


def shifts(n_tp):
    return [[(i, (i + shift) % n_tp) for i in range(n_tp)] for shift in range(1, n_tp)]


def send_blocks(part, n_tp, tp_idx):
    blocks = part.reshape(n_tp, part.shape[0] // n_tp, part.shape[1])
    pick = lambda i: lax.dynamic_index_in_dim(blocks, i % n_tp, 0, keepdims=False)
    return [pick(tp_idx)] + [lax.ppermute(pick(tp_idx + 1 + d), 'tp', perm) for d, perm in enumerate(shifts(n_tp))]


def send_total(blocks, n_tp):
    total = functools.reduce(jnp.add, blocks)
    return [total] + [lax.ppermute(total, 'tp', perm) for perm in shifts(n_tp)]


def join_totals(totals, n_tp, tp_idx):
    whole = jnp.zeros((n_tp,) + totals[0].shape, totals[0].dtype)
    for shift, total in enumerate(totals):
        whole = lax.dynamic_update_index_in_dim(whole, total, (tp_idx + n_tp - shift) % n_tp, 0)
    return whole.reshape(-1, totals[0].shape[1])


def solution(mesh):
    n_tp, n_dp = mesh.shape['tp'], mesh.shape['dp']

    def program(hidden, residual, targets, embedding, norm_w):
        inv_n = 1.0 / (hidden.shape[0] * hidden.shape[1])

        def local_part(hid_loc, res_loc, tgt_loc, emb_loc, norm_vec):
            n_batch, n_seq, d_model = hid_loc.shape
            n_rows = n_batch * n_seq
            vocab_loc = emb_loc.shape[0]
            tp_idx, dp_idx = lax.axis_index('tp'), lax.axis_index('dp')
            resid = (res_loc + hid_loc.astype(jnp.float32)).reshape(n_rows, d_model)
            tgt_rows = tgt_loc.reshape(n_rows)
            inv_rms = lax.rsqrt(jnp.mean(resid * resid, axis=-1, keepdims=True) + NORM_EPS)
            scaled_r = resid * inv_rms
            h_wide = lax.reduce_precision(scaled_r * norm_vec, exponent_bits=8, mantissa_bits=7)
            h_act = h_wide.astype(jnp.bfloat16)

            local_ids = (tgt_rows - tp_idx * vocab_loc)[:, None]
            local_ids = jnp.where(local_ids < vocab_loc, local_ids, -1)
            logits, max_loc, sum_loc, tgt_part = local_logits(h_act, emb_loc, local_ids)
            parts = lax.all_gather(jnp.stack([max_loc[:, 0], sum_loc[:, 0], tgt_part[:, 0]]), 'tp')
            row_max = jnp.max(parts[:, 0], axis=0)
            sum_exp = jnp.sum(parts[:, 1] * jnp.exp(parts[:, 0] - row_max), axis=0)
            loss_part = jnp.sum(row_max + jnp.log(sum_exp) - jnp.sum(parts[:, 2], axis=0)) * inv_n
            stats = jnp.zeros((8, d_model), jnp.float32)
            stats = stats.at[0, :n_rows].set(row_max).at[1, :n_rows].set(inv_n / sum_exp)
            stats = stats.at[2, :n_rows].set(tgt_rows.astype(jnp.float32))

            first = 0
            h_parts = []
            for c, n_tok in enumerate(TOKEN_CHUNKS):
                part = h_wide[first:first + n_tok]
                first += n_tok
                if c == STATS_CHUNK:
                    part = jnp.concatenate([part, stats])
                elif c > STATS_CHUNK:
                    part, _ = lax.optimization_barrier((part, stats))
                h_parts.append(lax.all_gather(part, 'dp'))
            all_stats = h_parts[STATS_CHUNK][:, TOKEN_CHUNKS[STATS_CHUNK]:, :n_rows]

            grad_h = local_grad_h(logits, emb_loc, local_ids, row_max[:, None], (inv_n / sum_exp)[:, None], inv_n)
            h_parts[0], grad_h = lax.optimization_barrier((h_parts[0], grad_h))
            grad_h = send_blocks(grad_h, n_tp, tp_idx)

            own_rows = sum(GRAD_CHUNKS)
            split_rows = n_dp * own_rows
            row_ids = (tp_idx * vocab_loc + jnp.arange(vocab_loc)).astype(jnp.float32)[:, None]
            own_emb, own_ids, base = [], [], 0
            for n_own in GRAD_CHUNKS:
                start = base + dp_idx * n_own
                own_emb.append(lax.dynamic_slice_in_dim(emb_loc, start, n_own))
                own_ids.append(lax.dynamic_slice_in_dim(row_ids, start, n_own))
                base += n_dp * n_own
            own_emb, own_ids = jnp.concatenate(own_emb), jnp.concatenate(own_ids)

            first_block = split_rows // ROW_BLOCK
            n_blocks = -(-vocab_loc // ROW_BLOCK) - first_block
            own, out, first = None, None, 0
            last = len(TOKEN_CHUNKS) - 1
            for c, n_tok in enumerate(TOKEN_CHUNKS):
                h_part = h_parts[c]
                if out is not None:
                    h_part, out = lax.optimization_barrier((h_part, out))
                h_chunk = cast_tokens(h_part, n_tok)
                chunk_stats = all_stats[:, :, first:first + n_tok].transpose(1, 0, 2).reshape(8, n_dp * n_tok)
                first += n_tok
                own = grad_rows(own_emb, own_ids, h_chunk, chunk_stats, own, inv_n, own_rows, 0, 1, own_rows)
                if c == last:
                    chunk_stats, own = lax.optimization_barrier((chunk_stats, own))
                out = grad_rows(emb_loc, row_ids, h_chunk, chunk_stats, out, inv_n,
                                vocab_loc, first_block, n_blocks, ROW_BLOCK)
                if c == 0:
                    grad_h, out = lax.optimization_barrier((grad_h, out))
                    grad_h = send_total(grad_h, n_tp)
                elif c == 1:
                    grad_h, out = lax.optimization_barrier((grad_h, out))
                    grad_h = join_totals(grad_h, n_tp, tp_idx)
                    grad_scaled = grad_h * norm_vec
                    grad_r = inv_rms * (grad_scaled - scaled_r * jnp.mean(grad_scaled * scaled_r, axis=-1, keepdims=True))
                    grad_w = jnp.sum(grad_h * scaled_r, axis=0)

            first, base = 0, 0
            for c, n_own in enumerate(GRAD_CHUNKS):
                part = own[first:first + n_own]
                first += n_own
                if c == len(GRAD_CHUNKS) - 1:
                    sums = jnp.zeros((8, d_model), jnp.float32).at[0].set(grad_w).at[1, 0].set(loss_part)
                    part = jnp.concatenate([part, sums])
                gathered = lax.all_gather(part, 'dp')
                out = place_rows(gathered, n_own, out, base)
                base += n_dp * n_own
            sums = jnp.sum(gathered[:, n_own:n_own + 2], axis=0)
            return sums[1, 0], grad_r.reshape(n_batch, n_seq, d_model), out, sums[0]

        sharded = jax.shard_map(
            local_part, mesh=mesh,
            in_specs=(P('dp', None, None), P('dp', None, None), P('dp', None), P('tp', None), P(None)),
            out_specs=(P(), P('dp', None, None), P('tp', None), P(None)),
            check_vma=False)
        return sharded(hidden, residual, targets, embedding, norm_w)

    return program
```

```python
import functools

import jax
import jax.numpy as jnp
from jax import lax
from jax.experimental import pallas as pl
from jax.experimental.pallas import tpu as pltpu
from jax.sharding import PartitionSpec as P


NORM_EPS = 1e-5
LANES = 128
VMEM_LIMIT = 60 * 1024 * 1024
NT = (((1,), (1,)), ((), ()))
SHARE_ROWS = 24
PIECES = (('share', 0, 24), ('direct', 96, 40), ('direct', 136, 40), ('direct', 176, 40), ('direct', 216, 40), ('stats', 256, 8))
PLAN = ((('start', 0), ('start', 1)), (), (), (('start', 2), ('r', 0, 1)), (), (), (('r', 1, 1),), (), (), (), (('r', 2, 1),),
 (('start', 5),), (('x', 1), ('r', 0, 2)), (), (), (), (), (('r', 1, 2), ('f', 1)), (), (),
 (('r', 2, 2), ('r', 5, 1), ('r', 0, 3), ('r', 1, 3), ('x', 2), ('start', 3), ('r', 2, 3), ('r', 5, 2), ('r', 0, 4),
  ('r', 1, 4), ('start', 4), ('r', 3, 1), ('x', 3), ('r', 2, 4), ('r', 5, 3), ('r', 4, 1), ('f', 2), ('x', 4),
  ('r', 3, 2), ('r', 5, 4), ('f', 3), ('f', 4), ('r', 4, 2), ('r', 3, 3), ('r', 4, 3), ('r', 3, 4), ('r', 4, 4)))
VOCAB_BLOCK = 1280
GRAD_CHUNKS = (256, 64)
ROW_BLOCK = 512
TOKEN_BLOCK = 1024
OWN_BLOCKS = 2


RING = 4
HOPS = {1: ((1, 0), (-1, 0), (0, 1), (0, -1)),
        2: ((2, 0), (0, 2), (1, 1), (1, -1), (-1, 1), (-1, -1)),
        3: ((1, 2), (-1, 2), (2, 1), (2, -1)),
        4: ((2, 2),)}


class Exchange:
    def __init__(self, own_ref, stats_ref, all_ref, sems, share_rows):
        self.own_ref, self.stats_ref, self.all_ref = own_ref, stats_ref, all_ref
        self.sems = sems
        self.n_rows = own_ref.shape[0]
        self.share_rows = share_rows
        width = own_ref.shape[1]
        self.quarter, self.half, self.width = width // 4, width // 2, width
        self.x = lax.axis_index('tp')
        dp = lax.axis_index('dp')
        self.core = lax.rem(dp, 2)
        self.y = lax.rem(dp // 2, RING)
        self.z = dp // (2 * RING)

    def at(self, dx=0, dy=0, dz=0, other=False):
        x = lax.rem(self.x + dx + RING, RING)
        y = lax.rem(self.y + dy + RING, RING)
        z = lax.rem(self.z + dz + RING, RING)
        core = 1 - self.core if other else self.core
        return (x, (z * RING + y) * 2 + core)

    def pos(self, hop):
        return lax.rem(self.z + hop[1] + RING, RING) * RING + lax.rem(self.y + hop[0] + RING, RING)

    def rows(self, piece):
        kind, start, size = piece
        if kind == 'share':
            start = pl.multiple_of(self.x * self.share_rows, 8)
        return pl.ds(start, size)

    def block(self, hop, rows, first=0, size=None):
        return self.all_ref.at[self.core, self.pos(hop), rows, pl.ds(first, size or self.width)]

    def send(self, src, dst, device, send, recv):
        pltpu.make_async_remote_copy(
            src_ref=src, dst_ref=dst, send_sem=self.sems[send], recv_sem=recv,
            device_id=device, device_id_type=pl.DeviceIdType.MESH).start()

    def barrier(self):
        sem = pltpu.get_barrier_semaphore()
        peers = [self.at(dx=1), self.at(dx=-1), self.at(dx=2), self.at(dy=1), self.at(dy=-1),
                 self.at(dz=1), self.at(dz=-1), self.at(other=True)]
        for peer in peers:
            pl.semaphore_signal(sem, inc=1, device_id=peer, device_id_type=pl.DeviceIdType.MESH)
        pl.semaphore_wait(sem, len(peers))

    def to_pair(self, src, dst):
        self.send(src, dst, self.at(other=True), 'pair_send', self.sems['pair_recv'])

    def start_own(self):
        dst = self.all_ref.at[self.core, self.pos((0, 0)), pl.ds(0, self.n_rows)]
        pltpu.make_async_copy(self.own_ref, dst, self.sems['local']).start()
        self.to_pair(self.own_ref, dst)

    def start_stats(self):
        dst = self.all_ref.at[self.core, self.pos((0, 0)), pl.ds(self.n_rows, 8)]
        pltpu.make_async_copy(self.stats_ref, dst, self.sems['local']).start()
        self.to_pair(self.stats_ref, dst)

    def plane(self, hop_src, rows, first, size, dy, dz, recv):
        ref = self.block(hop_src, rows, first, size)
        self.send(ref, ref, self.at(dy=dy, dz=dz), 'plane_send', recv)

    def round(self, p, piece, k):
        rows, recv = self.rows(piece), self.sems['plane_recv'].at[p, k - 1]
        q, h = self.quarter, self.half
        if k == 1:
            src = self.stats_ref if piece[0] == 'stats' else self.own_ref.at[rows]
            for dy, dz in HOPS[1]:
                self.send(src, self.block((0, 0), rows), self.at(dy=dy, dz=dz), 'plane_send', recv)
        elif k == 2:
            for s in (1, -1):
                for o in (1, -1):
                    self.plane((o, 0), rows, 0, h, 0, s, recv)
                    self.plane((0, o), rows, h, h, s, 0, recv)
            self.plane((-1, 0), rows, q, h, 1, 0, recv)
            self.plane((0, -1), rows, q, h, 0, 1, recv)
            for first in (0, 3 * q):
                self.plane((1, 0), rows, first, q, -1, 0, recv)
                self.plane((0, 1), rows, first, q, 0, -1, recv)
        elif k == 3:
            for s in (1, -1):
                self.plane((2, 0), rows, 0, h, 0, s, recv)
                self.plane((0, 2), rows, h, h, s, 0, recv)
            for o in (1, -1):
                self.plane((o, -1), rows, q, q, 0, 1, recv)
                self.plane((o, 1), rows, 0, q, 0, -1, recv)
                self.plane((-1, o), rows, h, q, 1, 0, recv)
                self.plane((1, o), rows, 3 * q, q, -1, 0, recv)
        else:
            self.plane((2, -1), rows, q, q, 0, 1, recv)
            self.plane((2, 1), rows, 0, q, 0, -1, recv)
            self.plane((-1, 2), rows, h, q, 1, 0, recv)
            self.plane((1, 2), rows, 3 * q, q, -1, 0, recv)

    def wait(self, ref, sem):
        pltpu.make_async_copy(ref, ref, sem).wait()

    def finish_round(self, p, piece, k):
        n, rows = len(HOPS[k]), self.rows(piece)
        self.wait(self.all_ref.at[0, pl.ds(0, n), pl.ds(0, piece[2])], self.sems['plane_recv'].at[p, k - 1])
        for hop in HOPS[k]:
            ref = self.block(hop, rows)
            self.to_pair(ref, ref)
            if piece[0] == 'share':
                for s in (1, -1):
                    self.send(ref, ref, self.at(dx=s), 'x_send', self.sems['x_recv'].at[k - 1])

    def share_of(self, dx):
        x = lax.rem(self.x + dx + RING, RING)
        return pl.ds(pl.multiple_of(x * self.share_rows, 8), self.share_rows)

    def along_x(self, k):
        n = len(HOPS[k])
        self.wait(self.all_ref.at[0, pl.ds(0, n), pl.ds(0, 2 * self.share_rows)], self.sems['x_recv'].at[k - 1])
        for hop in HOPS[k]:
            for dx, first in ((-1, 0), (1, self.half)):
                rows = self.share_of(dx)
                ref = self.block(hop, rows, first, self.half)
                self.send(ref, ref, self.at(dx=-dx), 'x_send', self.sems['far_recv'].at[k - 1])
                ref = self.block(hop, rows)
                self.to_pair(ref, ref)

    def finish_x(self, k):
        n, rows = len(HOPS[k]), self.share_of(2)
        self.wait(self.all_ref.at[0, pl.ds(0, n), pl.ds(0, self.share_rows)], self.sems['far_recv'].at[k - 1])
        for hop in HOPS[k]:
            ref = self.block(hop, rows)
            self.to_pair(ref, ref)

    def finish(self, pieces):
        n_other = RING * RING - 1
        total = sum(size for _, _, size in pieces)
        self.wait(self.all_ref.at[0], self.sems['pair_recv'])
        self.wait(self.all_ref.at[0], self.sems['pair_send'])
        self.wait(self.all_ref.at[0, pl.ds(0, n_other), pl.ds(0, total)], self.sems['plane_send'])
        self.wait(self.all_ref.at[0, pl.ds(0, n_other), pl.ds(0, 3 * self.share_rows)], self.sems['x_send'])
        self.wait(self.all_ref.at[0, 0], self.sems['local'])


def exchange_kernel(plan, pieces, share_rows, vocab, inv_n, h_ref, own_ref, emb_ref, ids_ref, tgt_ref,
                    all_ref, grad_ref, stats_out_ref, logits_ref, m_ref, s_ref, t_ref, col_ref, stats_ref, part_ref,
                    plane_recv, x_recv, far_recv, pair_recv, plane_send, x_send, pair_send, local, part_recv, part_send):
    step = pl.program_id(0)
    n_tiles, rows, width = logits_ref.shape
    sems = dict(plane_recv=plane_recv, x_recv=x_recv, far_recv=far_recv, pair_recv=pair_recv, plane_send=plane_send,
                x_send=x_send, pair_send=pair_send, local=local)
    ex = Exchange(own_ref, stats_ref, all_ref, sems, share_rows)

    def run(event):
        if event[0] == 'start':
            ex.round(event[1], pieces[event[1]], 1)
        elif event[0] == 'r':
            _, p, k = event
            ex.finish_round(p, pieces[p], k)
            if k < 4:
                ex.round(p, pieces[p], k + 1)
        elif event[0] == 'x':
            ex.along_x(event[1])
        else:
            ex.finish_x(event[1])

    for i, events in enumerate(plan):
        if events:
            @pl.when(step == i)
            def _(i=i, events=events):
                if i == 0:
                    ex.barrier()
                    ex.start_own()
                for event in events:
                    run(event)
                if i == len(plan) - 1:
                    ex.finish(pieces)

    @pl.when(step == 0)
    def _():
        m_ref[...] = jnp.full_like(m_ref, -jnp.inf)
        s_ref[...] = jnp.zeros_like(s_ref)
        t_ref[...] = jnp.zeros_like(t_ref)
        grad_ref[...] = jnp.zeros_like(grad_ref)

    @pl.when(step < n_tiles)
    def _():
        logits = lax.dot_general(h_ref[...], emb_ref[...], NT, preferred_element_type=jnp.float32)
        logits_ref[step] = logits
        lane = lax.broadcasted_iota(jnp.int32, (rows, LANES), 1)
        tgt_sum = t_ref[...]
        parts = []
        for j in range(width // LANES):
            ids = lane + (step * width + j * LANES)
            part = jnp.where(ids < vocab, logits[:, j * LANES:(j + 1) * LANES], -jnp.inf)
            tgt_sum += jnp.where(ids == ids_ref[...], part, 0.0)
            parts.append(part)
        t_ref[...] = tgt_sum
        m_old = m_ref[...]
        m_new = functools.reduce(jnp.maximum, parts, m_old)
        floor = jnp.where(m_new == -jnp.inf, 0.0, m_new)
        s_new = s_ref[...] * jnp.exp(m_old - floor)
        for part in parts:
            s_new += jnp.exp(part - floor)
        m_ref[...] = m_new
        s_ref[...] = s_new

    @pl.when(step == n_tiles)
    def _():
        m_col = jnp.max(m_ref[...], axis=1, keepdims=True)
        s_col = jnp.sum(s_ref[...] * jnp.exp(m_ref[...] - m_col), axis=1, keepdims=True)
        t_col = jnp.sum(t_ref[...], axis=1, keepdims=True)
        lane = lax.broadcasted_iota(jnp.int32, (rows, LANES), 1)
        cols = jnp.where(lane == 0, m_col, jnp.where(lane == 1, s_col, jnp.where(lane == 2, t_col, 0.0)))
        part_ref[ex.x] = cols.T[:8]
        for dx in (1, 2, 3):
            dst = part_ref.at[ex.x]
            pltpu.make_async_remote_copy(
                src_ref=dst, dst_ref=dst, send_sem=part_send, recv_sem=part_recv,
                device_id=ex.at(dx=dx), device_id_type=pl.DeviceIdType.MESH).start()
        ex.wait(part_ref.at[pl.ds(0, 3)], part_recv)
        ex.wait(part_ref.at[pl.ds(0, 3)], part_send)
        m_row = functools.reduce(jnp.maximum, [part_ref[i, 0:1] for i in range(RING)])
        s_row = sum(part_ref[i, 1:2] * jnp.exp(part_ref[i, 0:1] - m_row) for i in range(RING))
        t_row = sum(part_ref[i, 2:3] for i in range(RING))
        sub = lax.broadcasted_iota(jnp.int32, (8, rows), 0)
        values = (m_row, inv_n / s_row, tgt_ref[...], s_row, t_row)
        final = jnp.zeros((8, rows), jnp.float32)
        for i, value in enumerate(values):
            final = jnp.where(sub == i, value, final)
        stats_out_ref[...] = final
        stats_ref[...] = jnp.zeros_like(stats_ref)
        stats_ref[:, :rows] = final
        col_ref[...] = jnp.concatenate([final, jnp.zeros((LANES - 8, rows), jnp.float32)]).T
        ex.start_stats()

    def add_grad(masked):
        tile = step - n_tiles
        ids = lax.broadcasted_iota(jnp.int32, (rows, width), 1) + tile * width
        grad = jnp.exp(logits_ref[tile] - col_ref[:, 0:1]) * col_ref[:, 1:2]
        grad -= jnp.where(ids == ids_ref[...], inv_n, 0.0)
        emb = emb_ref[...]
        if masked:
            grad = jnp.where(ids < vocab, grad, 0.0)
            emb_ids = lax.broadcasted_iota(jnp.int32, emb.shape, 0) + tile * width
            emb = jnp.where(emb_ids < vocab, emb.astype(jnp.float32), 0.0).astype(emb.dtype)
        grad_ref[...] += jnp.dot(grad.astype(jnp.bfloat16), emb, preferred_element_type=jnp.float32)

    pl.when(jnp.logical_and(step >= n_tiles, step < 2 * n_tiles - 1))(lambda: add_grad(False))
    pl.when(step == 2 * n_tiles - 1)(lambda: add_grad(True))


def exchange_tokens(h_act, h_wide, emb, local_ids, tgt_row, inv_n, n_dp):
    rows, width = h_act.shape
    vocab = emb.shape[0]
    n_tiles = pl.cdiv(vocab, VOCAB_BLOCK)
    n_steps = 2 * n_tiles + 1
    plan = PLAN if len(PLAN) == n_steps else PLAN[:-1] + ((),) * (n_steps - len(PLAN)) + PLAN[-1:]
    dma = pltpu.SemaphoreType.DMA
    emb_tile = lambda i: (jnp.where(i < n_tiles, i, jnp.minimum(i - n_tiles, n_tiles - 1)), 0)
    whole = pl.BlockSpec(memory_space=pltpu.VMEM)
    return pl.pallas_call(
        functools.partial(exchange_kernel, plan, PIECES, SHARE_ROWS, vocab, inv_n),
        out_shape=(jax.ShapeDtypeStruct((2, n_dp // 2, rows + 8, width), jnp.float32),
                   jax.ShapeDtypeStruct((rows, width), jnp.float32),
                   jax.ShapeDtypeStruct((8, rows), jnp.float32)),
        grid=(n_steps,),
        in_specs=[whole, whole, pl.BlockSpec((VOCAB_BLOCK, width), emb_tile), whole, whole],
        out_specs=(pl.BlockSpec(memory_space=pl.ANY), whole, whole),
        scratch_shapes=[pltpu.VMEM((n_tiles, rows, VOCAB_BLOCK), jnp.float32)]
                       + [pltpu.VMEM((rows, LANES), jnp.float32)] * 4
                       + [pltpu.VMEM((8, width), jnp.float32), pltpu.VMEM((RING, 8, rows), jnp.float32)]
                       + [dma((len(PIECES), 4)), dma((4,)), dma((4,))] + [dma] * 7,
        compiler_params=pltpu.CompilerParams(
            vmem_limit_bytes=VMEM_LIMIT, collective_id=0, has_side_effects=True),
        cost_estimate=pl.CostEstimate(
            flops=60 * rows * vocab * width, bytes_accessed=vocab * 4 * width, transcendentals=2 * rows * vocab),
        name="exchange_tokens",
    )(h_act, h_wide, emb, local_ids, tgt_row)


def own_rows_kernel(inv_n, emb_ref, rid_ref, all_ref, h_ref, stats_ref, acc_ref):
    @pl.when(pl.program_id(0) == 0)
    def _():
        acc_ref[...] = jnp.zeros_like(acc_ref)

    blocks, rows = all_ref.shape[1], all_ref.shape[2] - 8
    h_blk = all_ref[0, :, :rows, :].reshape(blocks * rows, all_ref.shape[3]).astype(jnp.bfloat16)
    h_ref[...] = h_blk
    stats = jnp.concatenate([all_ref[0, i, rows:, :rows] for i in range(blocks)], axis=1)
    stats_ref[...] = stats
    logits = lax.dot_general(emb_ref[...], h_blk, NT, preferred_element_type=jnp.float32)
    prob = jnp.exp(logits - stats[0:1]) * stats[1:2]
    grad = prob - jnp.where(rid_ref[...] == stats[2:3], inv_n, 0.0)
    acc_ref[...] += jnp.dot(grad.astype(jnp.bfloat16), h_blk, preferred_element_type=jnp.float32)


def own_rows(emb, rid, gathered, inv_n):
    n_core, n_pos, n_in, width = gathered.shape
    n_own, n_tok = emb.shape[0], n_in - 8
    total = n_core * n_pos * n_tok
    per_core = n_pos // OWN_BLOCKS
    return pl.pallas_call(
        functools.partial(own_rows_kernel, inv_n),
        out_shape=(jax.ShapeDtypeStruct((total, width), jnp.bfloat16),
                   jax.ShapeDtypeStruct((8, total), jnp.float32),
                   jax.ShapeDtypeStruct((n_own, width), jnp.float32)),
        grid=(n_core * per_core,),
        in_specs=[pl.BlockSpec(memory_space=pltpu.VMEM), pl.BlockSpec(memory_space=pltpu.VMEM),
                  pl.BlockSpec((1, OWN_BLOCKS, n_in, width), lambda i: (i // per_core, lax.rem(i, per_core), 0, 0))],
        out_specs=(pl.BlockSpec((OWN_BLOCKS * n_tok, width), lambda i: (i, 0)),
                   pl.BlockSpec((8, OWN_BLOCKS * n_tok), lambda i: (0, i)),
                   pl.BlockSpec((n_own, width), lambda i: (0, 0))),
        compiler_params=pltpu.CompilerParams(vmem_limit_bytes=VMEM_LIMIT),
        cost_estimate=pl.CostEstimate(
            flops=4 * n_own * total * width, bytes_accessed=total * width * 6, transcendentals=n_own * total),
        name="own_rows",
    )(emb, rid, gathered)


def grad_rows_kernel(inv_n, emb_ref, rid_ref, h_ref, stats_ref, *refs):
    acc_ref = refs[-1]

    @pl.when(pl.program_id(1) == 0)
    def _():
        acc_ref[...] = jnp.zeros_like(acc_ref)

    h_blk = h_ref[...]
    logits = lax.dot_general(emb_ref[...], h_blk, NT, preferred_element_type=jnp.float32)
    prob = jnp.exp(logits - stats_ref[0:1, :]) * stats_ref[1:2, :]
    grad = prob - jnp.where(rid_ref[...] == stats_ref[2:3, :], inv_n, 0.0)
    acc_ref[...] += jnp.dot(grad.astype(jnp.bfloat16), h_blk, preferred_element_type=jnp.float32)


def grad_rows(emb, rid, h_all, stats, out, inv_n, n_out, first_block, n_blocks, row_block):
    width = emb.shape[1]
    n_tok = h_all.shape[0]
    tok_block = min(TOKEN_BLOCK, n_tok)
    in_specs = [
        pl.BlockSpec((row_block, width), lambda i, t: (i + first_block, 0)),
        pl.BlockSpec((row_block, 1), lambda i, t: (i + first_block, 0)),
        pl.BlockSpec((tok_block, width), lambda i, t: (t, 0)),
        pl.BlockSpec((8, tok_block), lambda i, t: (0, t)),
    ]
    args = [emb, rid, h_all, stats]
    if out is not None:
        in_specs.append(pl.BlockSpec(memory_space=pl.ANY))
        args.append(out)
    rows = n_blocks * row_block
    return pl.pallas_call(
        functools.partial(grad_rows_kernel, inv_n),
        out_shape=jax.ShapeDtypeStruct((n_out, width), jnp.float32),
        grid=(n_blocks, n_tok // tok_block),
        in_specs=in_specs,
        out_specs=pl.BlockSpec((row_block, width), lambda i, t: (i + first_block, 0)),
        input_output_aliases={4: 0} if out is not None else {},
        compiler_params=pltpu.CompilerParams(vmem_limit_bytes=VMEM_LIMIT),
        cost_estimate=pl.CostEstimate(
            flops=4 * rows * n_tok * width,
            bytes_accessed=rows * width * 6 + n_blocks * n_tok * width * 2,
            transcendentals=rows * n_tok),
        name="grad_rows",
    )(*args)


def place_kernel(src_ref, prev_ref, dst_ref):
    del prev_ref
    dst_ref[...] = src_ref[0, : dst_ref.shape[0], :]


def place_rows(gathered, n_rows, out, first_row):
    n_dev, n_in, width = gathered.shape
    first_block = first_row // n_rows
    return pl.pallas_call(
        place_kernel,
        out_shape=jax.ShapeDtypeStruct(out.shape, out.dtype),
        grid=(n_dev,),
        in_specs=[pl.BlockSpec((1, n_in, width), lambda i: (i, 0, 0)),
                  pl.BlockSpec(memory_space=pl.ANY)],
        out_specs=pl.BlockSpec((n_rows, width), lambda i: (i + first_block, 0)),
        input_output_aliases={1: 0},
        cost_estimate=pl.CostEstimate(
            flops=gathered.size * 80, bytes_accessed=gathered.size * 8, transcendentals=0),
        name="place_rows",
    )(gathered, out)


def shifts(n_tp):
    return [[(i, (i + shift) % n_tp) for i in range(n_tp)] for shift in range(1, n_tp)]


def send_blocks(part, n_tp, tp_idx):
    blocks = part.reshape(n_tp, part.shape[0] // n_tp, part.shape[1])
    pick = lambda i: lax.dynamic_index_in_dim(blocks, i % n_tp, 0, keepdims=False)
    return [pick(tp_idx)] + [lax.ppermute(pick(tp_idx + 1 + d), 'tp', perm) for d, perm in enumerate(shifts(n_tp))]


def send_total(blocks, n_tp):
    total = functools.reduce(jnp.add, blocks)
    return [total] + [lax.ppermute(total, 'tp', perm) for perm in shifts(n_tp)]


def join_totals(totals, n_tp, tp_idx):
    whole = jnp.zeros((n_tp,) + totals[0].shape, totals[0].dtype)
    for shift, total in enumerate(totals):
        whole = lax.dynamic_update_index_in_dim(whole, total, (tp_idx + n_tp - shift) % n_tp, 0)
    return whole.reshape(-1, totals[0].shape[1])


def solution(mesh):
    n_tp, n_dp = mesh.shape['tp'], mesh.shape['dp']

    def program(hidden, residual, targets, embedding, norm_w):
        inv_n = 1.0 / (hidden.shape[0] * hidden.shape[1])

        def local_part(hid_loc, res_loc, tgt_loc, emb_loc, norm_vec):
            n_batch, n_seq, d_model = hid_loc.shape
            n_rows = n_batch * n_seq
            vocab_loc = emb_loc.shape[0]
            tp_idx, dp_idx = lax.axis_index('tp'), lax.axis_index('dp')
            resid = (res_loc + hid_loc.astype(jnp.float32)).reshape(n_rows, d_model)
            tgt_rows = tgt_loc.reshape(n_rows)
            inv_rms = lax.rsqrt(jnp.mean(resid * resid, axis=-1, keepdims=True) + NORM_EPS)
            scaled_r = resid * inv_rms
            h_wide = lax.reduce_precision(scaled_r * norm_vec, exponent_bits=8, mantissa_bits=7)
            h_act = h_wide.astype(jnp.bfloat16)
            local_ids = (tgt_rows - tp_idx * vocab_loc)[:, None]
            local_ids = jnp.where(local_ids < vocab_loc, local_ids, -1)
            tgt_row = tgt_rows.astype(jnp.float32)[None]
            gathered, grad_h, stats = exchange_tokens(h_act, h_wide, emb_loc, local_ids, tgt_row, inv_n, n_dp)
            loss_part = jnp.sum(stats[0] + jnp.log(stats[3]) - stats[4]) * inv_n

            own_total = sum(GRAD_CHUNKS)
            split_rows = n_dp * own_total
            row_ids = (tp_idx * vocab_loc + jnp.arange(vocab_loc)).astype(jnp.float32)[:, None]
            own_emb, own_ids, base = [], [], 0
            for n_own in GRAD_CHUNKS:
                start = base + dp_idx * n_own
                own_emb.append(lax.dynamic_slice_in_dim(emb_loc, start, n_own))
                own_ids.append(lax.dynamic_slice_in_dim(row_ids, start, n_own))
                base += n_dp * n_own
            h_all, all_stats, own = own_rows(jnp.concatenate(own_emb), jnp.concatenate(own_ids), gathered, inv_n)
            grad_h, own = lax.optimization_barrier((grad_h, own))
            grad_h = send_blocks(grad_h, n_tp, tp_idx)

            first_block = split_rows // ROW_BLOCK
            n_blocks = -(-vocab_loc // ROW_BLOCK) - first_block
            out = None
            for c, n_part in enumerate((1, 1, n_blocks - 2)):
                out = grad_rows(emb_loc, row_ids, h_all, all_stats, out, inv_n, vocab_loc, first_block, n_part, ROW_BLOCK)
                first_block += n_part
                if c < 2:
                    grad_h, out = lax.optimization_barrier((grad_h, out))
                    grad_h = join_totals(grad_h, n_tp, tp_idx) if c else send_total(grad_h, n_tp)
            grad_scaled = grad_h * norm_vec
            grad_r = inv_rms * (grad_scaled - scaled_r * jnp.mean(grad_scaled * scaled_r, axis=-1, keepdims=True))
            grad_w = jnp.sum(grad_h * scaled_r, axis=0)

            first, base = 0, 0
            for c, n_own in enumerate(GRAD_CHUNKS):
                part = own[first:first + n_own]
                first += n_own
                if c == len(GRAD_CHUNKS) - 1:
                    sums = jnp.zeros((8, d_model), jnp.float32).at[0].set(grad_w).at[1, 0].set(loss_part)
                    part = jnp.concatenate([part, sums])
                got = lax.all_gather(part, 'dp')
                out = place_rows(got, n_own, out, base)
                base += n_dp * n_own
            sums = jnp.sum(got[:, n_own:n_own + 2], axis=0)
            return sums[1, 0], grad_r.reshape(n_batch, n_seq, d_model), out, sums[0]

        sharded = jax.shard_map(
            local_part, mesh=mesh,
            in_specs=(P('dp', None, None), P('dp', None, None), P('dp', None), P('tp', None), P(None)),
            out_specs=(P(), P('dp', None, None), P('tp', None), P(None)),
            check_vma=False)
        return sharded(hidden, residual, targets, embedding, norm_w)

    return program
```

```python
import functools

import jax
import jax.numpy as jnp
from jax import lax
from jax.experimental import pallas as pl
from jax.experimental.pallas import tpu as pltpu
from jax.sharding import PartitionSpec as P


NORM_EPS = 1e-5
LANES = 128
VMEM_LIMIT = 60 * 1024 * 1024
NT = (((1,), (1,)), ((), ()))
SHARE_ROWS = 24
PIECES = (('share', 0, 24), ('direct', 96, 40), ('direct', 136, 40), ('direct', 176, 40), ('direct', 216, 40), ('stats', 256, 8))
PLAN = (
    ('s0,s1',),
    (),
    (),
    ('s2,r01',),
    (),
    (),
    ('r11',),
    (),
    (),
    (),
    ('r21',),
    ('s5',),
    ('x1,r02',),
    (),
    (),
    (),
    (),
    ('r12,f1',),
    (),
    (),
    ('r22,r51,r03,r13,x2,s3,r23,r52,r04,r14,s4,r31,x3,r24', 'r53,r41,f2,x4,r32,r54,f3,f4,r42,r33,r43,r34,r44'),
)
VOCAB_BLOCK = 1280
GRAD_CHUNKS = (144, 96)
ROW_BLOCK = 512
BLOCK_CALLS = (1, 1, 1, 2)
TOKEN_BLOCK = 1024
POS_BLOCK = 2
PLACE_BLOCK = 4


RING = 4
HOPS = {1: ((1, 0), (-1, 0), (0, 1), (0, -1)),
        2: ((2, 0), (0, 2), (1, 1), (1, -1), (-1, 1), (-1, -1)),
        3: ((1, 2), (-1, 2), (2, 1), (2, -1)),
        4: ((2, 2),)}


class Exchange:
    def __init__(self, own_ref, stats_ref, all_ref, sems, share_rows):
        self.own_ref, self.stats_ref, self.all_ref = own_ref, stats_ref, all_ref
        self.sems = sems
        self.n_rows = own_ref.shape[0]
        self.share_rows = share_rows
        width = own_ref.shape[1]
        self.quarter, self.half, self.width = width // 4, width // 2, width
        self.x = lax.axis_index('tp')
        dp = lax.axis_index('dp')
        self.core = lax.rem(dp, 2)
        self.y = lax.rem(dp // 2, RING)
        self.z = dp // (2 * RING)

    def at(self, dx=0, dy=0, dz=0, other=False):
        x = lax.rem(self.x + dx + RING, RING)
        y = lax.rem(self.y + dy + RING, RING)
        z = lax.rem(self.z + dz + RING, RING)
        core = 1 - self.core if other else self.core
        return (x, (z * RING + y) * 2 + core)

    def pos(self, hop):
        return lax.rem(self.z + hop[1] + RING, RING) * RING + lax.rem(self.y + hop[0] + RING, RING)

    def rows(self, piece):
        kind, start, size = piece
        if kind == 'share':
            start = pl.multiple_of(self.x * self.share_rows, 8)
        return pl.ds(start, size)

    def block(self, hop, rows, first=0, size=None):
        return self.all_ref.at[self.core, self.pos(hop), rows, pl.ds(first, size or self.width)]

    def send(self, src, dst, device, send, recv):
        pltpu.make_async_remote_copy(
            src_ref=src, dst_ref=dst, send_sem=self.sems[send], recv_sem=recv,
            device_id=device, device_id_type=pl.DeviceIdType.MESH).start()

    def barrier(self):
        sem = pltpu.get_barrier_semaphore()
        peers = [self.at(dx=1), self.at(dx=-1), self.at(dx=2), self.at(dy=1), self.at(dy=-1),
                 self.at(dz=1), self.at(dz=-1), self.at(other=True)]
        for peer in peers:
            pl.semaphore_signal(sem, inc=1, device_id=peer, device_id_type=pl.DeviceIdType.MESH)
        pl.semaphore_wait(sem, len(peers))

    def to_pair(self, src, dst):
        self.send(src, dst, self.at(other=True), 'pair_send', self.sems['pair_recv'])

    def start_own(self):
        dst = self.all_ref.at[self.core, self.pos((0, 0)), pl.ds(0, self.n_rows)]
        pltpu.make_async_copy(self.own_ref, dst, self.sems['local']).start()
        self.to_pair(self.own_ref, dst)

    def start_stats(self):
        dst = self.all_ref.at[self.core, self.pos((0, 0)), pl.ds(self.n_rows, 8)]
        pltpu.make_async_copy(self.stats_ref, dst, self.sems['local']).start()
        self.to_pair(self.stats_ref, dst)

    def plane(self, hop_src, rows, first, size, dy, dz, recv):
        ref = self.block(hop_src, rows, first, size)
        self.send(ref, ref, self.at(dy=dy, dz=dz), 'plane_send', recv)

    def round(self, p, piece, k):
        rows, recv = self.rows(piece), self.sems['plane_recv'].at[p, k - 1]
        q, h = self.quarter, self.half
        if k == 1:
            src = self.stats_ref if piece[0] == 'stats' else self.own_ref.at[rows]
            for dy, dz in HOPS[1]:
                self.send(src, self.block((0, 0), rows), self.at(dy=dy, dz=dz), 'plane_send', recv)
        elif k == 2:
            for s in (1, -1):
                for o in (1, -1):
                    self.plane((o, 0), rows, 0, h, 0, s, recv)
                    self.plane((0, o), rows, h, h, s, 0, recv)
            self.plane((-1, 0), rows, q, h, 1, 0, recv)
            self.plane((0, -1), rows, q, h, 0, 1, recv)
            for first in (0, 3 * q):
                self.plane((1, 0), rows, first, q, -1, 0, recv)
                self.plane((0, 1), rows, first, q, 0, -1, recv)
        elif k == 3:
            for s in (1, -1):
                self.plane((2, 0), rows, 0, h, 0, s, recv)
                self.plane((0, 2), rows, h, h, s, 0, recv)
            for o in (1, -1):
                self.plane((o, -1), rows, q, q, 0, 1, recv)
                self.plane((o, 1), rows, 0, q, 0, -1, recv)
                self.plane((-1, o), rows, h, q, 1, 0, recv)
                self.plane((1, o), rows, 3 * q, q, -1, 0, recv)
        else:
            self.plane((2, -1), rows, q, q, 0, 1, recv)
            self.plane((2, 1), rows, 0, q, 0, -1, recv)
            self.plane((-1, 2), rows, h, q, 1, 0, recv)
            self.plane((1, 2), rows, 3 * q, q, -1, 0, recv)

    def wait(self, ref, sem):
        pltpu.make_async_copy(ref, ref, sem).wait()

    def finish_round(self, p, piece, k):
        n, rows = len(HOPS[k]), self.rows(piece)
        self.wait(self.all_ref.at[0, pl.ds(0, n), pl.ds(0, piece[2])], self.sems['plane_recv'].at[p, k - 1])
        for hop in HOPS[k]:
            ref = self.block(hop, rows)
            self.to_pair(ref, ref)
            if piece[0] == 'share':
                for s in (1, -1):
                    self.send(ref, ref, self.at(dx=s), 'x_send', self.sems['x_recv'].at[k - 1])

    def share_of(self, dx):
        x = lax.rem(self.x + dx + RING, RING)
        return pl.ds(pl.multiple_of(x * self.share_rows, 8), self.share_rows)

    def along_x(self, k):
        n = len(HOPS[k])
        self.wait(self.all_ref.at[0, pl.ds(0, n), pl.ds(0, 2 * self.share_rows)], self.sems['x_recv'].at[k - 1])
        for hop in HOPS[k]:
            for dx, first in ((-1, 0), (1, self.half)):
                rows = self.share_of(dx)
                ref = self.block(hop, rows, first, self.half)
                self.send(ref, ref, self.at(dx=-dx), 'x_send', self.sems['far_recv'].at[k - 1])
                ref = self.block(hop, rows)
                self.to_pair(ref, ref)

    def finish_x(self, k):
        n, rows = len(HOPS[k]), self.share_of(2)
        self.wait(self.all_ref.at[0, pl.ds(0, n), pl.ds(0, self.share_rows)], self.sems['far_recv'].at[k - 1])
        for hop in HOPS[k]:
            ref = self.block(hop, rows)
            self.to_pair(ref, ref)

    def finish(self, pieces):
        n_other = RING * RING - 1
        total = sum(size for _, _, size in pieces)
        self.wait(self.all_ref.at[0], self.sems['pair_recv'])
        self.wait(self.all_ref.at[0], self.sems['pair_send'])
        self.wait(self.all_ref.at[0, pl.ds(0, n_other), pl.ds(0, total)], self.sems['plane_send'])
        self.wait(self.all_ref.at[0, pl.ds(0, n_other), pl.ds(0, 3 * self.share_rows)], self.sems['x_send'])
        self.wait(self.all_ref.at[0, 0], self.sems['local'])


def exchange_kernel(plan, pieces, share_rows, vocab, inv_n, h_ref, own_ref, emb_ref, ids_ref, tgt_ref,
                    all_ref, grad_ref, stats_out_ref, logits_ref, m_ref, s_ref, t_ref, col_ref, stats_ref, part_ref,
                    plane_recv, x_recv, far_recv, pair_recv, plane_send, x_send, pair_send, local, part_recv, part_send):
    step = pl.program_id(0)
    n_tiles, rows, width = logits_ref.shape
    sems = dict(plane_recv=plane_recv, x_recv=x_recv, far_recv=far_recv, pair_recv=pair_recv, plane_send=plane_send,
                x_send=x_send, pair_send=pair_send, local=local)
    ex = Exchange(own_ref, stats_ref, all_ref, sems, share_rows)

    def run(event):
        kind, *nums = event
        nums = [int(v) for v in nums]
        if kind == 's':
            ex.round(nums[0], pieces[nums[0]], 1)
        elif kind == 'r':
            p, k = nums
            ex.finish_round(p, pieces[p], k)
            if k < 4:
                ex.round(p, pieces[p], k + 1)
        elif kind == 'x':
            ex.along_x(nums[0])
        else:
            ex.finish_x(nums[0])

    for i, groups in enumerate(plan):
        events = [event for group in groups for event in group.split(',')]
        if events:
            @pl.when(step == i)
            def _(i=i, events=events):
                if i == 0:
                    ex.barrier()
                    ex.start_own()
                for event in events:
                    run(event)
                if i == len(plan) - 1:
                    ex.finish(pieces)

    @pl.when(step == 0)
    def _():
        m_ref[...] = jnp.full_like(m_ref, -jnp.inf)
        s_ref[...] = jnp.zeros_like(s_ref)
        t_ref[...] = jnp.zeros_like(t_ref)
        grad_ref[...] = jnp.zeros_like(grad_ref)

    @pl.when(step < n_tiles)
    def _():
        logits = lax.dot_general(h_ref[...], emb_ref[...], NT, preferred_element_type=jnp.float32)
        logits_ref[step] = logits
        lane = lax.broadcasted_iota(jnp.int32, (rows, LANES), 1)
        tgt_sum = t_ref[...]
        parts = []
        for j in range(width // LANES):
            ids = lane + (step * width + j * LANES)
            part = jnp.where(ids < vocab, logits[:, j * LANES:(j + 1) * LANES], -jnp.inf)
            tgt_sum += jnp.where(ids == ids_ref[...], part, 0.0)
            parts.append(part)
        t_ref[...] = tgt_sum
        m_old = m_ref[...]
        m_new = functools.reduce(jnp.maximum, parts, m_old)
        floor = jnp.where(m_new == -jnp.inf, 0.0, m_new)
        s_new = s_ref[...] * jnp.exp(m_old - floor)
        for part in parts:
            s_new += jnp.exp(part - floor)
        m_ref[...] = m_new
        s_ref[...] = s_new

    @pl.when(step == n_tiles)
    def _():
        m_col = jnp.max(m_ref[...], axis=1, keepdims=True)
        s_col = jnp.sum(s_ref[...] * jnp.exp(m_ref[...] - m_col), axis=1, keepdims=True)
        t_col = jnp.sum(t_ref[...], axis=1, keepdims=True)
        lane = lax.broadcasted_iota(jnp.int32, (rows, LANES), 1)
        cols = jnp.where(lane == 0, m_col, jnp.where(lane == 1, s_col, jnp.where(lane == 2, t_col, 0.0)))
        part_ref[ex.x] = cols.T[:8]
        for dx in (1, 2, 3):
            dst = part_ref.at[ex.x]
            pltpu.make_async_remote_copy(
                src_ref=dst, dst_ref=dst, send_sem=part_send, recv_sem=part_recv,
                device_id=ex.at(dx=dx), device_id_type=pl.DeviceIdType.MESH).start()
        ex.wait(part_ref.at[pl.ds(0, 3)], part_recv)
        ex.wait(part_ref.at[pl.ds(0, 3)], part_send)
        m_row = functools.reduce(jnp.maximum, [part_ref[i, 0:1] for i in range(RING)])
        s_row = sum(part_ref[i, 1:2] * jnp.exp(part_ref[i, 0:1] - m_row) for i in range(RING))
        t_row = sum(part_ref[i, 2:3] for i in range(RING))
        sub = lax.broadcasted_iota(jnp.int32, (8, rows), 0)
        values = (m_row, inv_n / s_row, tgt_ref[...], s_row, t_row)
        final = jnp.zeros((8, rows), jnp.float32)
        for i, value in enumerate(values):
            final = jnp.where(sub == i, value, final)
        stats_out_ref[...] = final
        stats_ref[...] = jnp.zeros_like(stats_ref)
        stats_ref[:, :rows] = final
        col_ref[...] = jnp.concatenate([final, jnp.zeros((LANES - 8, rows), jnp.float32)]).T
        ex.start_stats()

    def add_grad(masked):
        tile = step - n_tiles
        ids = lax.broadcasted_iota(jnp.int32, (rows, width), 1) + tile * width
        grad = jnp.exp(logits_ref[tile] - col_ref[:, 0:1]) * col_ref[:, 1:2]
        grad -= jnp.where(ids == ids_ref[...], inv_n, 0.0)
        emb = emb_ref[...]
        if masked:
            grad = jnp.where(ids < vocab, grad, 0.0)
            emb_ids = lax.broadcasted_iota(jnp.int32, emb.shape, 0) + tile * width
            emb = jnp.where(emb_ids < vocab, emb.astype(jnp.float32), 0.0).astype(emb.dtype)
        grad_ref[...] += jnp.dot(grad.astype(jnp.bfloat16), emb, preferred_element_type=jnp.float32)

    pl.when(jnp.logical_and(step >= n_tiles, step < 2 * n_tiles - 1))(lambda: add_grad(False))
    pl.when(step == 2 * n_tiles - 1)(lambda: add_grad(True))


def exchange_tokens(h_act, h_wide, emb, local_ids, tgt_row, inv_n, n_dp):
    rows, width = h_act.shape
    vocab = emb.shape[0]
    n_tiles = pl.cdiv(vocab, VOCAB_BLOCK)
    n_steps = 2 * n_tiles + 1
    plan = PLAN if len(PLAN) == n_steps else PLAN[:-1] + ((),) * (n_steps - len(PLAN)) + PLAN[-1:]
    dma = pltpu.SemaphoreType.DMA
    emb_tile = lambda i: (jnp.where(i < n_tiles, i, jnp.minimum(i - n_tiles, n_tiles - 1)), 0)
    whole = pl.BlockSpec(memory_space=pltpu.VMEM)
    return pl.pallas_call(
        functools.partial(exchange_kernel, plan, PIECES, SHARE_ROWS, vocab, inv_n),
        out_shape=(jax.ShapeDtypeStruct((2, n_dp // 2, rows + 8, width), jnp.float32),
                   jax.ShapeDtypeStruct((rows, width), jnp.float32),
                   jax.ShapeDtypeStruct((8, rows), jnp.float32)),
        grid=(n_steps,),
        in_specs=[whole, whole, pl.BlockSpec((VOCAB_BLOCK, width), emb_tile), whole, whole],
        out_specs=(pl.BlockSpec(memory_space=pl.ANY), whole, whole),
        scratch_shapes=[pltpu.VMEM((n_tiles, rows, VOCAB_BLOCK), jnp.float32)]
                       + [pltpu.VMEM((rows, LANES), jnp.float32)] * 4
                       + [pltpu.VMEM((8, width), jnp.float32), pltpu.VMEM((RING, 8, rows), jnp.float32)]
                       + [dma((len(PIECES), 4)), dma((4,)), dma((4,))] + [dma] * 7,
        compiler_params=pltpu.CompilerParams(
            vmem_limit_bytes=VMEM_LIMIT, collective_id=0, has_side_effects=True),
        cost_estimate=pl.CostEstimate(
            flops=60 * rows * vocab * width, bytes_accessed=vocab * 4 * width, transcendentals=2 * rows * vocab),
        name="exchange_tokens",
    )(h_act, h_wide, emb, local_ids, tgt_row)


def row_grads(inv_n, emb, row_ids, h_blk, stats):
    logits = lax.dot_general(emb, h_blk, NT, preferred_element_type=jnp.float32)
    prob = jnp.exp(logits - stats[0:1]) * stats[1:2]
    grad = prob - jnp.where(row_ids == stats[2:3], inv_n, 0.0)
    return jnp.dot(grad.astype(jnp.bfloat16), h_blk, preferred_element_type=jnp.float32)


def id_column(n_rows, first):
    return (lax.broadcasted_iota(jnp.int32, (n_rows, 1), 0) + first).astype(jnp.float32)


def load_tokens(all_ref):
    blocks, rows = all_ref.shape[1], all_ref.shape[2] - 8
    h_blk = all_ref[0, :, :rows, :].reshape(blocks * rows, all_ref.shape[3]).astype(jnp.bfloat16)
    return h_blk, jnp.concatenate([all_ref[0, i, rows:, :rows] for i in range(blocks)], axis=1)


def token_spec(gathered):
    _, n_pos, n_in, width = gathered.shape
    per_core = n_pos // POS_BLOCK
    return pl.BlockSpec((1, POS_BLOCK, n_in, width), lambda i, where: (i // per_core, lax.rem(i, per_core), 0, 0))


def own_rows_kernel(inv_n, bases, where, emb0_ref, emb1_ref, all_ref, own0_ref, own1_ref, emb_ref, acc_ref):
    n0, n1 = emb0_ref.shape[0], emb1_ref.shape[0]

    @pl.when(pl.program_id(0) == 0)
    def _():
        emb_ref[:n0] = emb0_ref[...]
        emb_ref[n0:] = emb1_ref[...]
        acc_ref[...] = jnp.zeros_like(acc_ref)

    first0, first1 = [where[1] + base + where[0] * n for base, n in zip(bases, (n0, n1))]
    row = lax.broadcasted_iota(jnp.int32, (n0 + n1, 1), 0)
    row_ids = (row + jnp.where(row < n0, first0, first1 - n0)).astype(jnp.float32)
    h_blk, stats = load_tokens(all_ref)
    acc_ref[...] += row_grads(inv_n, emb_ref[...], row_ids, h_blk, stats)

    @pl.when(pl.program_id(0) == pl.num_programs(0) - 1)
    def _():
        own0_ref[...] = acc_ref[:n0]
        own1_ref[:n1] = acc_ref[n0:]
        own1_ref[n1:] = jnp.zeros_like(own1_ref[n1:])


def own_rows(emb, gathered, where, inv_n, n_dp):
    width = emb.shape[1]
    n_tok = gathered.shape[0] * gathered.shape[1] * (gathered.shape[2] - 8)
    n0, n1 = GRAD_CHUNKS
    bases = (0, n_dp * n0)
    emb_spec = lambda base, n: pl.BlockSpec((n, width), lambda i, where: (base // n + where[0], 0))
    whole = lambda n: pl.BlockSpec((n, width), lambda i, where: (0, 0))
    return pl.pallas_call(
        functools.partial(own_rows_kernel, inv_n, bases),
        out_shape=(jax.ShapeDtypeStruct((n0, width), jnp.float32), jax.ShapeDtypeStruct((n1 + 8, width), jnp.float32)),
        grid_spec=pltpu.PrefetchScalarGridSpec(
            num_scalar_prefetch=1,
            grid=(gathered.shape[0] * gathered.shape[1] // POS_BLOCK,),
            in_specs=[emb_spec(bases[0], n0), emb_spec(bases[1], n1), token_spec(gathered)],
            out_specs=(whole(n0), whole(n1 + 8)),
            scratch_shapes=[pltpu.VMEM((n0 + n1, width), jnp.bfloat16), pltpu.VMEM((n0 + n1, width), jnp.float32)]),
        compiler_params=pltpu.CompilerParams(vmem_limit_bytes=VMEM_LIMIT),
        cost_estimate=pl.CostEstimate(
            flops=4 * (n0 + n1) * n_tok * width, bytes_accessed=n_tok * width * 4, transcendentals=(n0 + n1) * n_tok),
        name="own_rows",
    )(where, emb, emb, gathered)


def first_block_kernel(inv_n, first, where, emb_ref, all_ref, out_ref, copy_ref, h_ref, stats_ref):
    step, last = pl.program_id(0), pl.num_programs(0) - 1

    @pl.when(step == 0)
    def _():
        out_ref[...] = jnp.zeros_like(out_ref)

    h_blk, stats = load_tokens(all_ref)
    h_ref[...] = h_blk
    stats_ref[...] = stats
    n_rows = emb_ref.shape[0]
    row_ids = id_column(n_rows, where[1] + (where[2] + first) * n_rows)
    out_ref[...] += row_grads(inv_n, emb_ref[...], row_ids, h_blk, stats)

    @pl.when(step == last)
    def _():
        copy_ref[...] = out_ref[...]


def first_block(emb, gathered, where, inv_n, first):
    vocab, width = emb.shape
    n_tok = gathered.shape[0] * gathered.shape[1] * (gathered.shape[2] - 8)
    per_step = POS_BLOCK * (gathered.shape[2] - 8)
    row_spec = pl.BlockSpec((ROW_BLOCK, width), lambda i, where: (first + where[2], 0))
    return pl.pallas_call(
        functools.partial(first_block_kernel, inv_n, first),
        out_shape=(jax.ShapeDtypeStruct((vocab, width), jnp.float32),
                   jax.ShapeDtypeStruct((ROW_BLOCK, width), jnp.float32),
                   jax.ShapeDtypeStruct((n_tok, width), jnp.bfloat16),
                   jax.ShapeDtypeStruct((8, n_tok), jnp.float32)),
        grid_spec=pltpu.PrefetchScalarGridSpec(
            num_scalar_prefetch=1,
            grid=(n_tok // per_step,),
            in_specs=[row_spec, token_spec(gathered)],
            out_specs=(row_spec, pl.BlockSpec((ROW_BLOCK, width), lambda i, where: (0, 0)),
                       pl.BlockSpec((per_step, width), lambda i, where: (i, 0)),
                       pl.BlockSpec((8, per_step), lambda i, where: (0, i)))),
        compiler_params=pltpu.CompilerParams(vmem_limit_bytes=VMEM_LIMIT),
        cost_estimate=pl.CostEstimate(
            flops=4 * ROW_BLOCK * n_tok * width, bytes_accessed=n_tok * width * 6, transcendentals=ROW_BLOCK * n_tok),
        name="first_block",
    )(where, emb, gathered)


class Placing:
    def __init__(self, out_ref, got_ref, recv_refs, recv_rows, n_steps, stages, sems):
        self.out_ref, self.got_ref, self.recv_refs, self.recv_rows = out_ref, got_ref, recv_refs, recv_rows
        self.n_steps, self.stages, self.sems = n_steps, stages, sems
        self.per_step = got_ref.shape[0] // n_steps
        self.n_got = stages[0].shape[2]
        self.n_recv = stages[1].shape[1]
        self.parts = recv_refs[0].shape[0] // self.n_recv

    def copies(self, step, slot, store):
        sem = self.sems.at[1 if store else 0, slot]
        for j in range(self.per_step):
            i = step * self.per_step + j
            stage = self.stages[0].at[slot, j]
            if store:
                yield pltpu.make_async_copy(stage, self.out_ref.at[pl.ds(pl.multiple_of(i * self.n_got, 8), self.n_got)], sem)
            else:
                yield pltpu.make_async_copy(self.got_ref.at[i, pl.ds(0, self.n_got)], stage, sem)

    def recv_copy(self, step, slot, store, k):
        sem = self.sems.at[3 if store else 2, slot]
        part = (step - k * self.parts) * self.n_recv
        stage = self.stages[1].at[slot]
        if store:
            row = pl.multiple_of(self.recv_rows[k] + part, 8)
            return pltpu.make_async_copy(stage, self.out_ref.at[pl.ds(row, self.n_recv)], sem)
        return pltpu.make_async_copy(self.recv_refs[k].at[pl.ds(pl.multiple_of(part, 8), self.n_recv)], stage, sem)

    def each(self, step, store, act):
        slot = lax.rem(step, 2)
        for copy in self.copies(step, slot, store):
            act(copy)
        for k in range(len(self.recv_refs)):
            @pl.when(jnp.logical_and(step >= k * self.parts, step < (k + 1) * self.parts))
            def _(k=k):
                act(self.recv_copy(step, slot, store, k))

    def before(self, step):
        @pl.when(step >= 1)
        def _():
            self.each(step - 1, False, lambda c: c.wait())
            self.each(step - 1, True, lambda c: c.start())

        @pl.when(step >= 2)
        def _():
            self.each(step - 2, True, lambda c: c.wait())

        self.each(step, False, lambda c: c.start())

    def after(self, step):
        @pl.when(step == self.n_steps - 1)
        def _():
            self.each(step, False, lambda c: c.wait())
            self.each(step, True, lambda c: c.start())
            self.each(step - 1, True, lambda c: c.wait())
            self.each(step, True, lambda c: c.wait())


def grad_rows_kernel(inv_n, first, n_steps, recv_firsts, where, emb_ref, h_ref, stats_ref, *refs):
    i, t = pl.program_id(0), pl.program_id(1)
    n_ref = 2 + len(recv_firsts) if recv_firsts else 1
    out_in_ref, acc_ref, copy_ref = refs[0], refs[n_ref], refs[n_ref + 1]
    n_rows = emb_ref.shape[0]
    placing = None
    if recv_firsts:
        rows = [(where[3] + block) * n_rows for block in recv_firsts]
        placing = Placing(out_in_ref, refs[1], refs[2:n_ref], rows, n_steps, refs[n_ref + 2:n_ref + 4], refs[n_ref + 4])
        placing.before(i * pl.num_programs(1) + t)

    @pl.when(t == 0)
    def _():
        acc_ref[...] = jnp.zeros_like(acc_ref)

    row_ids = id_column(n_rows, where[1] + (where[2] + first + i) * n_rows)
    acc_ref[...] += row_grads(inv_n, emb_ref[...], row_ids, h_ref[...], stats_ref[...])

    @pl.when(t == pl.num_programs(1) - 1)
    def _():
        copy_ref[...] = acc_ref[...]

    if placing:
        placing.after(i * pl.num_programs(1) + t)


def grad_rows(emb, h_all, stats, where, out, inv_n, first, n_blocks, got=None, n_got=0, recvs=(), recv_firsts=()):
    vocab, width = emb.shape
    n_tok = h_all.shape[0]
    tok_block = min(TOKEN_BLOCK, n_tok)
    n_steps = n_blocks * (n_tok // tok_block)
    row_spec = pl.BlockSpec((ROW_BLOCK, width), lambda i, t, where: (i + first + where[2], 0))
    anywhere = pl.BlockSpec(memory_space=pl.ANY)
    in_specs = [row_spec, pl.BlockSpec((tok_block, width), lambda i, t, where: (t, 0)),
                pl.BlockSpec((8, tok_block), lambda i, t, where: (0, t)), anywhere]
    args, scratch = [emb, h_all, stats, out], []
    if recvs:
        args += [got, *recvs]
        in_specs += [anywhere] * (1 + len(recvs))
        part = ROW_BLOCK * len(recvs) // n_steps
        part = next(n for n in range(max(part, 8), ROW_BLOCK + 1, 8) if ROW_BLOCK % n == 0 and n * n_steps >= ROW_BLOCK * len(recvs))
        scratch = [pltpu.VMEM((2, got.shape[0] // n_steps, n_got, width), jnp.float32),
                   pltpu.VMEM((2, part, width), jnp.float32), pltpu.SemaphoreType.DMA((4, 2))]
    rows = n_blocks * ROW_BLOCK
    return pl.pallas_call(
        functools.partial(grad_rows_kernel, inv_n, first, n_steps, tuple(recv_firsts)),
        out_shape=(jax.ShapeDtypeStruct((vocab, width), jnp.float32), jax.ShapeDtypeStruct((rows, width), jnp.float32)),
        grid_spec=pltpu.PrefetchScalarGridSpec(
            num_scalar_prefetch=1,
            grid=(n_blocks, n_tok // tok_block),
            in_specs=in_specs,
            out_specs=(row_spec, pl.BlockSpec((ROW_BLOCK, width), lambda i, t, where: (i, 0))),
            scratch_shapes=scratch),
        input_output_aliases={4: 0},
        compiler_params=pltpu.CompilerParams(vmem_limit_bytes=VMEM_LIMIT),
        cost_estimate=pl.CostEstimate(
            flops=4 * rows * n_tok * width,
            bytes_accessed=rows * width * 6 + n_blocks * n_tok * width * 2,
            transcendentals=rows * n_tok),
        name="grad_rows",
    )(where, *args)


def place_kernel(where, src_ref, prev_ref, dst_ref):
    del where, prev_ref
    n_dev, n_rows = src_ref.shape[0], dst_ref.shape[0] // src_ref.shape[0]
    for i in range(n_dev):
        dst_ref[i * n_rows:(i + 1) * n_rows] = src_ref[i, :n_rows]


def place_rows(src, n_rows, out, where, first_block, per_block):
    n_src, n_in, width = src.shape
    return pl.pallas_call(
        place_kernel,
        out_shape=jax.ShapeDtypeStruct(out.shape, out.dtype),
        grid_spec=pltpu.PrefetchScalarGridSpec(
            num_scalar_prefetch=1,
            grid=(n_src // per_block,),
            in_specs=[pl.BlockSpec((per_block, n_in, width), lambda i, where: (i, 0, 0)),
                      pl.BlockSpec(memory_space=pl.ANY)],
            out_specs=pl.BlockSpec((per_block * n_rows, width), lambda i, where: (i + first_block + where[3], 0))),
        input_output_aliases={2: 0},
        compiler_params=pltpu.CompilerParams(vmem_limit_bytes=VMEM_LIMIT),
        cost_estimate=pl.CostEstimate(flops=src.size * 80, bytes_accessed=src.size * 8, transcendentals=0),
        name="place_rows",
    )(where, src, out)


def shifts(n_tp):
    return [[(i, (i + shift) % n_tp) for i in range(n_tp)] for shift in range(1, n_tp)]


def send_blocks(part, n_tp, tp_idx):
    blocks = part.reshape(n_tp, part.shape[0] // n_tp, part.shape[1])
    pick = lambda i: lax.dynamic_index_in_dim(blocks, i % n_tp, 0, keepdims=False)
    return [pick(tp_idx)] + [lax.ppermute(pick(tp_idx + 1 + d), 'tp', perm) for d, perm in enumerate(shifts(n_tp))]


def send_total(blocks, n_tp):
    total = functools.reduce(jnp.add, blocks)
    return [total] + [lax.ppermute(total, 'tp', perm) for perm in shifts(n_tp)]


def join_totals(totals, n_tp, tp_idx):
    whole = jnp.zeros((n_tp,) + totals[0].shape, totals[0].dtype)
    for shift, total in enumerate(totals):
        whole = lax.dynamic_update_index_in_dim(whole, total, (tp_idx + n_tp - shift) % n_tp, 0)
    return whole.reshape(-1, totals[0].shape[1])


def solution(mesh):
    n_tp, n_dp = mesh.shape['tp'], mesh.shape['dp']

    def program(hidden, residual, targets, embedding, norm_w):
        inv_n = 1.0 / (hidden.shape[0] * hidden.shape[1])

        def local_part(hid_loc, res_loc, tgt_loc, emb_loc, norm_vec):
            n_batch, n_seq, d_model = hid_loc.shape
            n_rows = n_batch * n_seq
            vocab_loc = emb_loc.shape[0]
            tp_idx, dp_idx = lax.axis_index('tp'), lax.axis_index('dp')
            resid = (res_loc + hid_loc.astype(jnp.float32)).reshape(n_rows, d_model)
            tgt_rows = tgt_loc.reshape(n_rows)
            inv_rms = lax.rsqrt(jnp.mean(resid * resid, axis=-1, keepdims=True) + NORM_EPS)
            scaled_r = resid * inv_rms
            h_wide = lax.reduce_precision(scaled_r * norm_vec, exponent_bits=8, mantissa_bits=7)
            h_act = h_wide.astype(jnp.bfloat16)
            local_ids = (tgt_rows - tp_idx * vocab_loc)[:, None]
            local_ids = jnp.where(local_ids < vocab_loc, local_ids, -1)
            tgt_row = tgt_rows.astype(jnp.float32)[None]
            gathered, grad_h, stats = exchange_tokens(h_act, h_wide, emb_loc, local_ids, tgt_row, inv_n, n_dp)
            loss_part = jnp.sum(stats[0] + jnp.log(stats[3]) - stats[4]) * inv_n

            per_core = sum(BLOCK_CALLS)
            core = dp_idx % 2
            where = jnp.stack([dp_idx, tp_idx * vocab_loc, core * per_core, (1 - core) * per_core]).astype(jnp.int32)
            own0, own1 = own_rows(emb_loc, gathered, where, inv_n, n_dp)
            got0 = lax.all_gather(own0, 'dp')
            gathered, grad_h, own0 = lax.optimization_barrier((gathered, grad_h, own0))
            grad_h = send_blocks(grad_h, n_tp, tp_idx)

            first = n_dp * sum(GRAD_CHUNKS) // ROW_BLOCK
            pair = [(i, i ^ 1) for i in range(n_dp)]
            out, copied, h_all, all_stats = first_block(emb_loc, gathered, where, inv_n, first)
            recvs, recv_firsts, late, block = [], [], [], first
            for c, n_blocks in enumerate(BLOCK_CALLS):
                final = c == len(BLOCK_CALLS) - 1
                if c:
                    extra = (got0, GRAD_CHUNKS[0], recvs, recv_firsts) if final else ()
                    out, copied = grad_rows(emb_loc, h_all, all_stats, where, out, inv_n, block, n_blocks, *extra)
                if c < 2:
                    grad_h, out = lax.optimization_barrier((grad_h, out))
                    grad_h = join_totals(grad_h, n_tp, tp_idx) if c else send_total(grad_h, n_tp)
                recv = lax.ppermute(copied, 'dp', pair)
                if c < len(BLOCK_CALLS) - 2:
                    recvs.append(recv)
                    recv_firsts.append(block)
                else:
                    late.append((recv, block))
                block += n_blocks
                if c == 1:
                    grad_scaled = grad_h * norm_vec
                    grad_r = inv_rms * (grad_scaled - scaled_r * jnp.mean(grad_scaled * scaled_r, axis=-1, keepdims=True))
                    grad_w = jnp.sum(grad_h * scaled_r, axis=0)
                    own1 = own1.at[-8].set(grad_w).at[-7, 0].set(loss_part)
                    got1 = lax.all_gather(own1, 'dp')

            n_own = GRAD_CHUNKS[1]
            n_place = PLACE_BLOCK * n_own
            (recv, block), (last_recv, last_block) = late
            out = place_rows(recv.reshape(-1, ROW_BLOCK, d_model), ROW_BLOCK, out, where, block, 1)
            out = place_rows(got1, n_own, out, jnp.zeros_like(where), n_dp * GRAD_CHUNKS[0] // n_place, PLACE_BLOCK)
            out = place_rows(last_recv.reshape(-1, ROW_BLOCK, d_model), ROW_BLOCK, out, where, last_block, 1)
            sums = jnp.sum(got1[:, n_own:n_own + 2], axis=0)
            return sums[1, 0], grad_r.reshape(n_batch, n_seq, d_model), out, sums[0]

        sharded = jax.shard_map(
            local_part, mesh=mesh,
            in_specs=(P('dp', None, None), P('dp', None, None), P('dp', None), P('tp', None), P(None)),
            out_specs=(P(), P('dp', None, None), P('tp', None), P(None)),
            check_vma=False)
        return sharded(hidden, residual, targets, embedding, norm_w)

    return program
```

```python
import functools
import itertools

import jax
import jax.numpy as jnp
from jax import lax
from jax.experimental import pallas as pl
from jax.experimental.pallas import tpu as pltpu
from jax.sharding import PartitionSpec as P


NORM_EPS = 1e-5
LANES = 128
VMEM_LIMIT = 60 << 20
NT = (((1,), (1,)), ((), ()))
SHARE_ROWS = 24
DIRECT_ROWS = 40
PIECES = (('share', 0, SHARE_ROWS),)
PIECES += tuple(('direct', 4 * SHARE_ROWS + i * DIRECT_ROWS, DIRECT_ROWS) for i in range(4))
PIECES += (('stats', 0, 8),)
PLAN = (
    ('s0,s1',),
    (),
    (),
    ('s2',),
    ('r01',),
    (),
    (),
    ('r11',),
    (),
    (),
    ('r21',),
    ('s5',),
    (),
    ('r02,x1',),
    (),
    (),
    (),
    (),
    ('r12',),
    (),
    ('r22,r51,r03,x2,s3,r13,f1,r23,r52,r04,s4,r31,r14,r24', 'r53,x3,r41,f2,r32,r54,x4,f3,r42,f4,r33,r43,r34,r44'),
)
VOCAB_BLOCK = 1280
GRAD_CHUNKS = (208, 64)
ROW_BLOCK = 512
BLOCK_CALLS = (1, 1, 1, 1)
TOKEN_BLOCK = 1024
POS_BLOCK = 2
OWN_POS_BLOCK = 4
PLACE_BLOCK = 4


RING = 4
SEMS = ('plane_recv', 'x_recv', 'far_recv', 'plane_send', 'x_send', 'pair_send', 'pair_recv', 'local')
SEMS += ('plane_send_stats', 'pair_send_stats', 'pair_recv_stats', 'local_stats')
HOPS = {k: [hop for hop in itertools.product((0, 1, 2, -1), repeat=2) if sum(map(abs, hop)) == k] for k in range(1, 5)}

SENDS = (('100201,10020-,-00201,-0020-,012210,0122-0,0-2210,0-22-0',
          '-01210,0-1201,1001-0,01010-,1031-0,01310-'),
         ('200201,20020-,022210,0222-0,1-1101,11010-,-12110,1131-0',
          '--1101,-1010-,--2110,1-31-0'),
         ('2-1101,21010-,-22110,1231-0',))


class Exchange:
    def __init__(self, own_ref, stats_ref, all_ref, all_stats_ref, sems, share_rows):
        self.own_ref, self.stats_ref, self.all_ref, self.all_stats_ref = own_ref, stats_ref, all_ref, all_stats_ref
        self.sems = sems
        self.share_rows = share_rows
        self.x = lax.axis_index('tp')
        dp = lax.axis_index('dp')
        self.core = lax.rem(dp, 2)
        self.y = lax.rem(dp // 2, RING)
        self.z = dp // (2 * RING)

    def at(self, dx=0, dy=0, dz=0, other=False):
        x = lax.rem(self.x + dx + RING, RING)
        y = lax.rem(self.y + dy + RING, RING)
        z = lax.rem(self.z + dz + RING, RING)
        core = 1 - self.core if other else self.core
        return (x, (z * RING + y) * 2 + core)

    def pos(self, hop):
        return lax.rem(self.z + hop[1] + RING, RING) * RING + lax.rem(self.y + hop[0] + RING, RING)

    def rows(self, piece):
        kind, start, size = piece
        if kind == 'share':
            start = pl.multiple_of(self.x * self.share_rows, 8)
        return pl.ds(start, size)

    def whole(self, piece):
        return self.all_stats_ref if piece[0] == 'stats' else self.all_ref

    def block(self, piece, hop, rows, first=0, size=4):
        ref = self.whole(piece)
        quarter = ref.shape[3] // 4
        return ref.at[self.core, self.pos(hop), rows, pl.ds(first * quarter, size * quarter)]

    def send(self, src, dst, device, send, recv):
        pltpu.make_async_remote_copy(
            src_ref=src, dst_ref=dst, send_sem=self.sems[send], recv_sem=recv,
            device_id=device, device_id_type=pl.DeviceIdType.MESH).start()

    def barrier(self):
        sem = pltpu.get_barrier_semaphore()
        peers = [self.at(dx=1), self.at(dx=-1), self.at(dx=2), self.at(dy=1), self.at(dy=-1),
                 self.at(dz=1), self.at(dz=-1), self.at(other=True)]
        for peer in peers:
            pl.semaphore_signal(sem, inc=1, device_id=peer, device_id_type=pl.DeviceIdType.MESH)
        pl.semaphore_wait(sem, len(peers))

    def to_pair(self, piece, src, dst):
        end = '_stats' if piece[0] == 'stats' else ''
        self.send(src, dst, self.at(other=True), 'pair_send' + end, self.sems['pair_recv' + end])

    def start_own(self, piece):
        stats = piece[0] == 'stats'
        src = self.stats_ref if stats else self.own_ref
        dst = self.whole(piece).at[self.core, self.pos((0, 0))]
        pltpu.make_async_copy(src, dst, self.sems['local_stats' if stats else 'local']).start()
        self.to_pair(piece, src, dst)

    def round(self, p, piece, k):
        rows, recv = self.rows(piece), self.sems['plane_recv'].at[p, k - 1]
        sent = 'plane_send_stats' if piece[0] == 'stats' else 'plane_send'

        def pass_on(hop, first, size, dy, dz):
            ref = self.block(piece, hop, rows, first, size)
            self.send(ref, ref, self.at(dy=dy, dz=dz), sent, recv)

        if k == 1:
            src = self.stats_ref if piece[0] == 'stats' else self.own_ref.at[rows]
            for dy, dz in HOPS[1]:
                self.send(src, self.block(piece, (0, 0), rows), self.at(dy=dy, dz=dz), sent, recv)
        else:
            for code in ','.join(SENDS[k - 2]).split(','):
                y, z, first, size, dy, dz = ['-0123'.index(c) - 1 for c in code]
                pass_on((y, z), first, size, dy, dz)

    def wait(self, ref, sem):
        pltpu.make_async_copy(ref, ref, sem).wait()

    def finish_round(self, p, piece, k):
        n, rows = len(HOPS[k]), self.rows(piece)
        self.wait(self.whole(piece).at[0, pl.ds(0, n), pl.ds(0, piece[2])], self.sems['plane_recv'].at[p, k - 1])
        for hop in HOPS[k]:
            ref = self.block(piece, hop, rows)
            self.to_pair(piece, ref, ref)
            if piece[0] == 'share':
                for s in (1, -1):
                    self.send(ref, ref, self.at(dx=s), 'x_send', self.sems['x_recv'].at[k - 1])

    def share_of(self, dx):
        x = lax.rem(self.x + dx + RING, RING)
        return pl.ds(pl.multiple_of(x * self.share_rows, 8), self.share_rows)

    def along_x(self, k):
        n, share = len(HOPS[k]), PIECES[0]
        self.wait(self.all_ref.at[0, pl.ds(0, n), pl.ds(0, 2 * self.share_rows)], self.sems['x_recv'].at[k - 1])
        for hop in HOPS[k]:
            for dx, first in ((-1, 0), (1, 2)):
                rows = self.share_of(dx)
                ref = self.block(share, hop, rows, first, 2)
                self.send(ref, ref, self.at(dx=-dx), 'x_send', self.sems['far_recv'].at[k - 1])
                ref = self.block(share, hop, rows)
                self.to_pair(share, ref, ref)

    def finish_x(self, k):
        n, share, rows = len(HOPS[k]), PIECES[0], self.share_of(2)
        self.wait(self.all_ref.at[0, pl.ds(0, n), pl.ds(0, self.share_rows)], self.sems['far_recv'].at[k - 1])
        for hop in HOPS[k]:
            ref = self.block(share, hop, rows)
            self.to_pair(share, ref, ref)

    def finish(self, pieces):
        others = pl.ds(0, RING * RING - 1)
        total = sum(size for kind, _, size in pieces if kind != 'stats')
        for end, ref in (('', self.all_ref), ('_stats', self.all_stats_ref)):
            self.wait(ref.at[0], self.sems['pair_recv' + end])
            self.wait(ref.at[0], self.sems['pair_send' + end])
            self.wait(ref.at[0, 0], self.sems['local' + end])
        self.wait(self.all_ref.at[0, others, pl.ds(0, total)], self.sems['plane_send'])
        self.wait(self.all_stats_ref.at[0, others], self.sems['plane_send_stats'])
        self.wait(self.all_ref.at[0, others, pl.ds(0, 3 * self.share_rows)], self.sems['x_send'])


def exchange_kernel(plan, pieces, share_rows, vocab, inv_n, h_ref, own_ref, emb_ref, ids_ref, tgt_ref,
                    all_ref, all_stats_ref, grad_ref, stats_out_ref,
                    logits_ref, m_ref, s_ref, t_ref, col_ref, stats_ref, part_ref, part_recv, part_send, *sem_refs):
    step = pl.program_id(0)
    n_tiles, rows, width = logits_ref.shape
    ex = Exchange(own_ref, stats_ref, all_ref, all_stats_ref, dict(zip(SEMS, sem_refs)), share_rows)

    def run(event):
        kind, *nums = event
        nums = [int(v) for v in nums]
        if kind == 's':
            ex.round(nums[0], pieces[nums[0]], 1)
        elif kind == 'r':
            p, k = nums
            ex.finish_round(p, pieces[p], k)
            if k < 4:
                ex.round(p, pieces[p], k + 1)
        elif kind == 'x':
            ex.along_x(nums[0])
        else:
            ex.finish_x(nums[0])

    for i, groups in enumerate(plan):
        events = [event for group in groups for event in group.split(',')]
        if events:
            @pl.when(step == i)
            def _(i=i, events=events):
                if i == 0:
                    ex.barrier()
                    ex.start_own(pieces[0])
                for event in events:
                    run(event)
                if i == len(plan) - 1:
                    ex.finish(pieces)

    @pl.when(step == 0)
    def _():
        m_ref[...] = jnp.full_like(m_ref, -jnp.inf)
        s_ref[...] = jnp.zeros_like(s_ref)
        t_ref[...] = jnp.zeros_like(t_ref)
        grad_ref[...] = jnp.zeros_like(grad_ref)

    @pl.when(step < n_tiles)
    def _():
        logits = lax.dot_general(h_ref[...], emb_ref[...], NT, preferred_element_type=jnp.float32)
        logits_ref[step] = logits
        lane = lax.broadcasted_iota(jnp.int32, (rows, LANES), 1)
        tgt_sum = t_ref[...]
        parts = []
        for j in range(width // LANES):
            ids = lane + (step * width + j * LANES)
            part = jnp.where(ids < vocab, logits[:, j * LANES:(j + 1) * LANES], -jnp.inf)
            tgt_sum += jnp.where(ids == ids_ref[...], part, 0.0)
            parts.append(part)
        t_ref[...] = tgt_sum
        m_old = m_ref[...]
        m_new = functools.reduce(jnp.maximum, parts, m_old)
        floor = jnp.where(m_new == -jnp.inf, 0.0, m_new)
        s_new = s_ref[...] * jnp.exp(m_old - floor)
        for part in parts:
            s_new += jnp.exp(part - floor)
        m_ref[...] = m_new
        s_ref[...] = s_new

    @pl.when(step == n_tiles)
    def _():
        m_col = jnp.max(m_ref[...], axis=1, keepdims=True)
        s_col = jnp.sum(s_ref[...] * jnp.exp(m_ref[...] - m_col), axis=1, keepdims=True)
        t_col = jnp.sum(t_ref[...], axis=1, keepdims=True)
        lane = lax.broadcasted_iota(jnp.int32, (rows, LANES), 1)
        cols = jnp.where(lane == 0, m_col, jnp.where(lane == 1, s_col, jnp.where(lane == 2, t_col, 0.0)))
        part_ref[ex.x] = cols.T[:8]
        for dx in (1, 2, 3):
            dst = part_ref.at[ex.x]
            pltpu.make_async_remote_copy(
                src_ref=dst, dst_ref=dst, send_sem=part_send, recv_sem=part_recv,
                device_id=ex.at(dx=dx), device_id_type=pl.DeviceIdType.MESH).start()
        ex.wait(part_ref.at[pl.ds(0, 3)], part_recv)
        ex.wait(part_ref.at[pl.ds(0, 3)], part_send)
        m_row = functools.reduce(jnp.maximum, [part_ref[i, 0:1] for i in range(RING)])
        s_row = sum(part_ref[i, 1:2] * jnp.exp(part_ref[i, 0:1] - m_row) for i in range(RING))
        t_row = sum(part_ref[i, 2:3] for i in range(RING))
        sub = lax.broadcasted_iota(jnp.int32, (8, rows), 0)
        values = (m_row, inv_n / s_row, tgt_ref[...], s_row, t_row)
        final = jnp.zeros((8, rows), jnp.float32)
        for i, value in enumerate(values):
            final = jnp.where(sub == i, value, final)
        stats_out_ref[...] = final
        stats_ref[...] = jnp.zeros_like(stats_ref)
        stats_ref[:, :rows] = final
        col_ref[...] = jnp.concatenate([final, jnp.zeros((LANES - 8, rows), jnp.float32)]).T
        ex.start_own(pieces[-1])

    def add_grad(masked):
        tile = step - n_tiles
        ids = lax.broadcasted_iota(jnp.int32, (rows, width), 1) + tile * width
        grad = jnp.exp(logits_ref[tile] - col_ref[:, 0:1]) * col_ref[:, 1:2]
        grad -= jnp.where(ids == ids_ref[...], inv_n, 0.0)
        if masked:
            grad = jnp.where(ids < vocab, grad, 0.0)
        grad = grad.astype(jnp.bfloat16)
        n_cols = grad_ref.shape[1] // 4

        @pl.loop(0, 4)
        def _(j):
            cols = pl.ds(pl.multiple_of(j * n_cols, LANES), n_cols)
            emb = emb_ref[:, cols]
            if masked:
                emb_ids = lax.broadcasted_iota(jnp.int32, emb.shape, 0) + tile * width
                emb = jnp.where(emb_ids < vocab, emb.astype(jnp.float32), 0.0).astype(emb.dtype)
            grad_ref[:, cols] += jnp.dot(grad, emb, preferred_element_type=jnp.float32)

    pl.when(jnp.logical_and(step >= n_tiles, step < 2 * n_tiles - 1))(lambda: add_grad(False))
    pl.when(step == 2 * n_tiles - 1)(lambda: add_grad(True))


def exchange_tokens(h_act, h_wide, emb, local_ids, tgt_row, inv_n, n_dp):
    rows, width = h_act.shape
    vocab = emb.shape[0]
    n_tiles = pl.cdiv(vocab, VOCAB_BLOCK)
    n_steps = 2 * n_tiles + 1
    plan = PLAN if len(PLAN) == n_steps else PLAN[:-1] + ((),) * (n_steps - len(PLAN)) + PLAN[-1:]
    dma = pltpu.SemaphoreType.DMA
    emb_tile = lambda i: (jnp.where(i < n_tiles, i, jnp.minimum(i - n_tiles, n_tiles - 1)), 0)
    whole = pl.BlockSpec(memory_space=pltpu.VMEM)
    return pl.pallas_call(
        functools.partial(exchange_kernel, plan, PIECES, SHARE_ROWS, vocab, inv_n),
        out_shape=(jax.ShapeDtypeStruct((2, n_dp // 2, rows, width), jnp.float32),
                   jax.ShapeDtypeStruct((2, n_dp // 2, 8, 4 * LANES), jnp.float32),
                   jax.ShapeDtypeStruct((rows, width), jnp.float32),
                   jax.ShapeDtypeStruct((8, rows), jnp.float32)),
        grid=(n_steps,),
        in_specs=[whole, whole, pl.BlockSpec((VOCAB_BLOCK, width), emb_tile), whole, whole],
        out_specs=(pl.BlockSpec(memory_space=pl.ANY), pl.BlockSpec(memory_space=pl.ANY), whole, whole),
        scratch_shapes=[pltpu.VMEM((n_tiles, rows, VOCAB_BLOCK), jnp.float32)]
                       + [pltpu.VMEM((rows, LANES), jnp.float32)] * 4
                       + [pltpu.VMEM((8, 4 * LANES), jnp.float32), pltpu.VMEM((RING, 8, rows), jnp.float32)]
                       + [dma, dma, dma((len(PIECES), 4)), dma((4,)), dma((4,))] + [dma] * (len(SEMS) - 3),
        compiler_params=pltpu.CompilerParams(
            vmem_limit_bytes=VMEM_LIMIT, collective_id=0, has_side_effects=True),
        cost_estimate=pl.CostEstimate(
            flops=60 * rows * vocab * width, bytes_accessed=vocab * 4 * width, transcendentals=2 * rows * vocab),
        name="exchange_tokens",
    )(h_act, h_wide, emb, local_ids, tgt_row)


def row_grads(inv_n, emb, row_ids, h_blk, stats):
    logits = lax.dot_general(emb, h_blk, NT, preferred_element_type=jnp.float32)
    prob = jnp.exp(logits - stats[0:1]) * stats[1:2]
    grad = prob - jnp.where(row_ids == stats[2:3], inv_n, 0.0)
    return jnp.dot(grad.astype(jnp.bfloat16), h_blk, preferred_element_type=jnp.float32)


def id_column(n_rows, first):
    return (lax.broadcasted_iota(jnp.int32, (n_rows, 1), 0) + first).astype(jnp.float32)


def load_tokens(all_ref, all_stats_ref):
    _, blocks, rows, width = all_ref.shape
    h_blk = all_ref[0].reshape(blocks * rows, width).astype(jnp.bfloat16)
    return h_blk, jnp.concatenate([all_stats_ref[0, i, :, :rows] for i in range(blocks)], axis=1)


def token_specs(gathered, pos_block):
    return [pl.BlockSpec((1, pos_block) + arr.shape[2:],
                         lambda i, where: (i * pos_block // arr.shape[1], lax.rem(i, arr.shape[1] // pos_block), 0, 0))
            for arr in gathered]


def own_rows_kernel(inv_n, bases, where, emb0_ref, emb1_ref, all_ref, all_stats_ref, own0_ref, own1_ref, emb_ref, acc_ref):
    n0, n1 = emb0_ref.shape[0], emb1_ref.shape[0]

    @pl.when(pl.program_id(0) == 0)
    def _():
        emb_ref[:n0] = emb0_ref[...]
        emb_ref[n0:] = emb1_ref[...]
        acc_ref[...] = jnp.zeros_like(acc_ref)

    first0, first1 = [where[1] + base + where[0] * n for base, n in zip(bases, (n0, n1))]
    row = lax.broadcasted_iota(jnp.int32, (n0 + n1, 1), 0)
    row_ids = (row + jnp.where(row < n0, first0, first1 - n0)).astype(jnp.float32)
    h_blk, stats = load_tokens(all_ref, all_stats_ref)
    acc_ref[...] += row_grads(inv_n, emb_ref[...], row_ids, h_blk, stats)

    @pl.when(pl.program_id(0) == pl.num_programs(0) - 1)
    def _():
        own0_ref[...] = acc_ref[:n0]
        own1_ref[:n1] = acc_ref[n0:]
        own1_ref[n1:] = jnp.zeros_like(own1_ref[n1:])


def own_rows(emb, gathered, where, inv_n, n_dp):
    width = emb.shape[1]
    n_tok = gathered[0].size // width
    n0, n1 = GRAD_CHUNKS
    bases = (0, n_dp * n0)
    emb_spec = lambda base, n: pl.BlockSpec((n, width), lambda i, where: (base // n + where[0], 0))
    whole = lambda n: pl.BlockSpec((n, width), lambda i, where: (0, 0))
    return pl.pallas_call(
        functools.partial(own_rows_kernel, inv_n, bases),
        out_shape=(jax.ShapeDtypeStruct((n0, width), jnp.float32), jax.ShapeDtypeStruct((n1 + 8, width), jnp.float32)),
        grid_spec=pltpu.PrefetchScalarGridSpec(
            num_scalar_prefetch=1,
            grid=(gathered[0].shape[0] * gathered[0].shape[1] // OWN_POS_BLOCK,),
            in_specs=[emb_spec(bases[0], n0), emb_spec(bases[1], n1)] + token_specs(gathered, OWN_POS_BLOCK),
            out_specs=(whole(n0), whole(n1 + 8)),
            scratch_shapes=[pltpu.VMEM((n0 + n1, width), jnp.bfloat16), pltpu.VMEM((n0 + n1, width), jnp.float32)]),
        compiler_params=pltpu.CompilerParams(vmem_limit_bytes=VMEM_LIMIT),
        cost_estimate=pl.CostEstimate(
            flops=4 * (n0 + n1) * n_tok * width, bytes_accessed=n_tok * width * 4, transcendentals=(n0 + n1) * n_tok),
        name="own_rows",
    )(where, emb, emb, *gathered)


def first_block_kernel(inv_n, first, where, emb_ref, all_ref, all_stats_ref, out_ref, copy_ref, h_ref, stats_ref):
    step, last = pl.program_id(0), pl.num_programs(0) - 1

    @pl.when(step == 0)
    def _():
        out_ref[...] = jnp.zeros_like(out_ref)

    h_blk, stats = load_tokens(all_ref, all_stats_ref)
    h_ref[...] = h_blk
    stats_ref[...] = stats
    n_rows = emb_ref.shape[0]
    row_ids = id_column(n_rows, where[1] + (where[2] + first) * n_rows)
    out_ref[...] += row_grads(inv_n, emb_ref[...], row_ids, h_blk, stats)

    @pl.when(step == last)
    def _():
        copy_ref[...] = out_ref[...]


def first_block(emb, gathered, where, inv_n, first):
    vocab, width = emb.shape
    n_tok = gathered[0].size // width
    per_step = POS_BLOCK * gathered[0].shape[2]
    row_spec = pl.BlockSpec((ROW_BLOCK, width), lambda i, where: (first + where[2], 0))
    return pl.pallas_call(
        functools.partial(first_block_kernel, inv_n, first),
        out_shape=(jax.ShapeDtypeStruct((vocab, width), jnp.float32),
                   jax.ShapeDtypeStruct((ROW_BLOCK, width), jnp.float32),
                   jax.ShapeDtypeStruct((n_tok, width), jnp.bfloat16),
                   jax.ShapeDtypeStruct((8, n_tok), jnp.float32)),
        grid_spec=pltpu.PrefetchScalarGridSpec(
            num_scalar_prefetch=1,
            grid=(n_tok // per_step,),
            in_specs=[row_spec] + token_specs(gathered, POS_BLOCK),
            out_specs=(row_spec, pl.BlockSpec((ROW_BLOCK, width), lambda i, where: (0, 0)),
                       pl.BlockSpec((per_step, width), lambda i, where: (i, 0)),
                       pl.BlockSpec((8, per_step), lambda i, where: (0, i)))),
        compiler_params=pltpu.CompilerParams(vmem_limit_bytes=VMEM_LIMIT),
        cost_estimate=pl.CostEstimate(
            flops=4 * ROW_BLOCK * n_tok * width, bytes_accessed=n_tok * width * 6, transcendentals=ROW_BLOCK * n_tok),
        name="first_block",
    )(where, emb, *gathered)


class Placing:
    def __init__(self, out_ref, got_ref, recv_refs, recv_rows, n_steps, stages, sems):
        self.out_ref, self.got_ref, self.recv_refs, self.recv_rows = out_ref, got_ref, recv_refs, recv_rows
        self.n_steps, self.stages, self.sems = n_steps, stages, sems
        self.per_step = got_ref.shape[0] // n_steps
        self.n_got = stages[0].shape[2]
        self.n_recv = stages[1].shape[1]
        self.parts = recv_refs[0].shape[0] // self.n_recv

    def copies(self, step, slot, store):
        sem = self.sems.at[1 if store else 0, slot]
        for j in range(self.per_step):
            i = step * self.per_step + j
            stage = self.stages[0].at[slot, j]
            if store:
                yield pltpu.make_async_copy(stage, self.out_ref.at[pl.ds(pl.multiple_of(i * self.n_got, 8), self.n_got)], sem)
            else:
                yield pltpu.make_async_copy(self.got_ref.at[i, pl.ds(0, self.n_got)], stage, sem)

    def recv_copy(self, step, slot, store, k):
        sem = self.sems.at[3 if store else 2, slot]
        part = (step - k * self.parts) * self.n_recv
        stage = self.stages[1].at[slot]
        if store:
            row = pl.multiple_of(self.recv_rows[k] + part, 8)
            return pltpu.make_async_copy(stage, self.out_ref.at[pl.ds(row, self.n_recv)], sem)
        return pltpu.make_async_copy(self.recv_refs[k].at[pl.ds(pl.multiple_of(part, 8), self.n_recv)], stage, sem)

    def each(self, step, store, act):
        slot = lax.rem(step, 2)
        for copy in self.copies(step, slot, store):
            act(copy)
        for k in range(len(self.recv_refs)):
            @pl.when(jnp.logical_and(step >= k * self.parts, step < (k + 1) * self.parts))
            def _(k=k):
                act(self.recv_copy(step, slot, store, k))

    def before(self, step):
        @pl.when(step >= 1)
        def _():
            self.each(step - 1, False, lambda c: c.wait())
            self.each(step - 1, True, lambda c: c.start())

        @pl.when(step >= 2)
        def _():
            self.each(step - 2, True, lambda c: c.wait())

        self.each(step, False, lambda c: c.start())

    def after(self, step):
        @pl.when(step == self.n_steps - 1)
        def _():
            self.each(step, False, lambda c: c.wait())
            self.each(step, True, lambda c: c.start())
            self.each(step - 1, True, lambda c: c.wait())
            self.each(step, True, lambda c: c.wait())


def grad_rows_kernel(inv_n, first, n_steps, recv_firsts, where, emb_ref, h_ref, stats_ref, *refs):
    i, t = pl.program_id(0), pl.program_id(1)
    n_ref = 2 + len(recv_firsts) if recv_firsts else 1
    out_in_ref, acc_ref, copy_ref = refs[0], refs[n_ref], refs[n_ref + 1]
    n_rows = emb_ref.shape[0]
    placing = None
    if recv_firsts:
        rows = [(where[3] + block) * n_rows for block in recv_firsts]
        placing = Placing(out_in_ref, refs[1], refs[2:n_ref], rows, n_steps, refs[n_ref + 2:n_ref + 4], refs[n_ref + 4])
        placing.before(i * pl.num_programs(1) + t)

    @pl.when(t == 0)
    def _():
        acc_ref[...] = jnp.zeros_like(acc_ref)

    row_ids = id_column(n_rows, where[1] + (where[2] + first + i) * n_rows)
    acc_ref[...] += row_grads(inv_n, emb_ref[...], row_ids, h_ref[...], stats_ref[...])

    @pl.when(t == pl.num_programs(1) - 1)
    def _():
        copy_ref[...] = acc_ref[...]

    if placing:
        placing.after(i * pl.num_programs(1) + t)


def grad_rows(emb, h_all, stats, where, out, inv_n, first, n_blocks, got=None, n_got=0, recvs=(), recv_firsts=()):
    vocab, width = emb.shape
    n_tok = h_all.shape[0]
    tok_block = min(TOKEN_BLOCK, n_tok)
    n_steps = n_blocks * (n_tok // tok_block)
    row_spec = pl.BlockSpec((ROW_BLOCK, width), lambda i, t, where: (i + first + where[2], 0))
    anywhere = pl.BlockSpec(memory_space=pl.ANY)
    in_specs = [row_spec, pl.BlockSpec((tok_block, width), lambda i, t, where: (t, 0)),
                pl.BlockSpec((8, tok_block), lambda i, t, where: (0, t)), anywhere]
    args, scratch = [emb, h_all, stats, out], []
    if recvs:
        args += [got, *recvs]
        in_specs += [anywhere] * (1 + len(recvs))
        part = ROW_BLOCK * len(recvs) // n_steps
        part = next(n for n in range(max(part, 8), ROW_BLOCK + 1, 8) if ROW_BLOCK % n == 0 and n * n_steps >= ROW_BLOCK * len(recvs))
        scratch = [pltpu.VMEM((2, got.shape[0] // n_steps, n_got, width), jnp.float32),
                   pltpu.VMEM((2, part, width), jnp.float32), pltpu.SemaphoreType.DMA((4, 2))]
    rows = n_blocks * ROW_BLOCK
    return pl.pallas_call(
        functools.partial(grad_rows_kernel, inv_n, first, n_steps, tuple(recv_firsts)),
        out_shape=(jax.ShapeDtypeStruct((vocab, width), jnp.float32), jax.ShapeDtypeStruct((rows, width), jnp.float32)),
        grid_spec=pltpu.PrefetchScalarGridSpec(
            num_scalar_prefetch=1,
            grid=(n_blocks, n_tok // tok_block),
            in_specs=in_specs,
            out_specs=(row_spec, pl.BlockSpec((ROW_BLOCK, width), lambda i, t, where: (i, 0))),
            scratch_shapes=scratch),
        input_output_aliases={4: 0},
        compiler_params=pltpu.CompilerParams(vmem_limit_bytes=VMEM_LIMIT),
        cost_estimate=pl.CostEstimate(
            flops=4 * rows * n_tok * width,
            bytes_accessed=rows * width * 6 + n_blocks * n_tok * width * 2,
            transcendentals=rows * n_tok),
        name="grad_rows",
    )(where, *args)


def place_kernel(where, src_ref, prev_ref, dst_ref):
    del where, prev_ref
    n_dev, n_rows = src_ref.shape[0], dst_ref.shape[0] // src_ref.shape[0]
    for i in range(n_dev):
        dst_ref[i * n_rows:(i + 1) * n_rows] = src_ref[i, :n_rows]


def place_rows(src, n_rows, out, where, first_block, per_block):
    n_src, n_in, width = src.shape
    return pl.pallas_call(
        place_kernel,
        out_shape=jax.ShapeDtypeStruct(out.shape, out.dtype),
        grid_spec=pltpu.PrefetchScalarGridSpec(
            num_scalar_prefetch=1,
            grid=(n_src // per_block,),
            in_specs=[pl.BlockSpec((per_block, n_in, width), lambda i, where: (i, 0, 0)),
                      pl.BlockSpec(memory_space=pl.ANY)],
            out_specs=pl.BlockSpec((per_block * n_rows, width), lambda i, where: (i + first_block + where[3], 0))),
        input_output_aliases={2: 0},
        compiler_params=pltpu.CompilerParams(vmem_limit_bytes=VMEM_LIMIT),
        cost_estimate=pl.CostEstimate(flops=src.size * 80, bytes_accessed=src.size * 8, transcendentals=0),
        name="place_rows",
    )(where, src, out)


def shifts(n_tp):
    return [[(i, (i + shift) % n_tp) for i in range(n_tp)] for shift in range(1, n_tp)]


def send_blocks(part, n_tp, tp_idx):
    blocks = part.reshape(n_tp, part.shape[0] // n_tp, part.shape[1])
    pick = lambda i: lax.dynamic_index_in_dim(blocks, i % n_tp, 0, keepdims=False)
    return [pick(tp_idx)] + [lax.ppermute(pick(tp_idx + 1 + d), 'tp', perm) for d, perm in enumerate(shifts(n_tp))]


def send_total(blocks, n_tp):
    total = functools.reduce(jnp.add, blocks)
    return [total] + [lax.ppermute(total, 'tp', perm) for perm in shifts(n_tp)]


def join_totals(totals, n_tp, tp_idx):
    whole = jnp.zeros((n_tp,) + totals[0].shape, totals[0].dtype)
    for shift, total in enumerate(totals):
        whole = lax.dynamic_update_index_in_dim(whole, total, (tp_idx + n_tp - shift) % n_tp, 0)
    return whole.reshape(-1, totals[0].shape[1])


def solution(mesh):
    n_tp, n_dp = mesh.shape['tp'], mesh.shape['dp']

    def program(hidden, residual, targets, embedding, norm_w):
        inv_n = 1.0 / (hidden.shape[0] * hidden.shape[1])

        def local_part(hid_loc, res_loc, tgt_loc, emb_loc, norm_vec):
            n_batch, n_seq, d_model = hid_loc.shape
            n_rows = n_batch * n_seq
            vocab_loc = emb_loc.shape[0]
            tp_idx, dp_idx = lax.axis_index('tp'), lax.axis_index('dp')
            resid = (res_loc + hid_loc.astype(jnp.float32)).reshape(n_rows, d_model)
            tgt_rows = tgt_loc.reshape(n_rows)
            inv_rms = lax.rsqrt(jnp.mean(resid * resid, axis=-1, keepdims=True) + NORM_EPS)
            scaled_r = resid * inv_rms
            h_wide = lax.reduce_precision(scaled_r * norm_vec, exponent_bits=8, mantissa_bits=7)
            h_act = h_wide.astype(jnp.bfloat16)
            local_ids = (tgt_rows - tp_idx * vocab_loc)[:, None]
            local_ids = jnp.where(local_ids < vocab_loc, local_ids, -1)
            tgt_row = tgt_rows.astype(jnp.float32)[None]
            *gathered, grad_h, stats = exchange_tokens(h_act, h_wide, emb_loc, local_ids, tgt_row, inv_n, n_dp)
            loss_part = jnp.sum(stats[0] + jnp.log(stats[3]) - stats[4]) * inv_n

            per_core = sum(BLOCK_CALLS)
            core = dp_idx % 2
            where = jnp.stack([dp_idx, tp_idx * vocab_loc, core * per_core, (1 - core) * per_core]).astype(jnp.int32)
            own0, own1 = own_rows(emb_loc, gathered, where, inv_n, n_dp)
            got0 = lax.all_gather(own0, 'dp')
            gathered, grad_h, own0 = lax.optimization_barrier((gathered, grad_h, own0))
            grad_h = send_blocks(grad_h, n_tp, tp_idx)

            first = n_dp * sum(GRAD_CHUNKS) // ROW_BLOCK
            pair = [(i, i ^ 1) for i in range(n_dp)]
            out, copied, h_all, all_stats = first_block(emb_loc, gathered, where, inv_n, first)
            recvs, recv_firsts, late, block = [], [], [], first
            for c, n_blocks in enumerate(BLOCK_CALLS):
                final = c == len(BLOCK_CALLS) - 1
                if c:
                    extra = (got0, GRAD_CHUNKS[0], recvs, recv_firsts) if final else ()
                    out, copied = grad_rows(emb_loc, h_all, all_stats, where, out, inv_n, block, n_blocks, *extra)
                if c < 2:
                    grad_h, out = lax.optimization_barrier((grad_h, out))
                    grad_h = join_totals(grad_h, n_tp, tp_idx) if c else send_total(grad_h, n_tp)
                recv = lax.ppermute(copied, 'dp', pair)
                if c < len(BLOCK_CALLS) - 2:
                    recvs.append(recv)
                    recv_firsts.append(block)
                else:
                    late.append((recv, block))
                block += n_blocks
                if c == 1:
                    grad_scaled = grad_h * norm_vec
                    grad_r = inv_rms * (grad_scaled - scaled_r * jnp.mean(grad_scaled * scaled_r, axis=-1, keepdims=True))
                    grad_w = jnp.sum(grad_h * scaled_r, axis=0)
                    own1 = own1.at[-8].set(grad_w).at[-7, 0].set(loss_part)
                    got1 = lax.all_gather(own1, 'dp')

            n_own = GRAD_CHUNKS[1]
            n_place = PLACE_BLOCK * n_own
            (recv, block), (last_recv, last_block) = late
            out = place_rows(recv.reshape(-1, ROW_BLOCK, d_model), ROW_BLOCK, out, where, block, 1)
            out = place_rows(got1, n_own, out, jnp.zeros_like(where), n_dp * GRAD_CHUNKS[0] // n_place, PLACE_BLOCK)
            out = place_rows(last_recv.reshape(-1, ROW_BLOCK, d_model), ROW_BLOCK, out, where, last_block, 1)
            sums = jnp.sum(got1[:, n_own:n_own + 2], axis=0)
            return sums[1, 0], grad_r.reshape(n_batch, n_seq, d_model), out, sums[0]

        sharded = jax.shard_map(
            local_part, mesh=mesh,
            in_specs=(P('dp', None, None), P('dp', None, None), P('dp', None), P('tp', None), P(None)),
            out_specs=(P(), P('dp', None, None), P('tp', None), P(None)),
            check_vma=False)
        return sharded(hidden, residual, targets, embedding, norm_w)

    return program
```

```python
import functools
import itertools

import jax
import jax.numpy as jnp
from jax import lax
from jax.experimental import pallas as pl
from jax.experimental.pallas import tpu as pltpu
from jax.sharding import PartitionSpec as P


NORM_EPS = 1e-5
LANES = 128
VMEM_LIMIT = 60 << 20
NT = (((1,), (1,)), ((), ()))
SHARE_ROWS = 24
DIRECT_ROWS = 40
PIECES = (('share', 0, SHARE_ROWS),)
PIECES += tuple(('direct', 4 * SHARE_ROWS + i * DIRECT_ROWS, DIRECT_ROWS) for i in range(4))
PIECES += (('stats', 0, 8),)
PLAN = (
    ('s0,s1',),
    (),
    (),
    ('s2',),
    ('r01',),
    (),
    (),
    ('r11',),
    (),
    (),
    ('r21',),
    ('s5',),
    (),
    ('r02,x1',),
    (),
    (),
    (),
    (),
    ('r12',),
    (),
    ('r22,r51,r03,x2,s3,r13,f1,r23,r52,r04,s4,r31,r14,r24', 'r53,x3,r41,f2,r32,r54,x4,f3,r42,f4,r33,r43,r34,r44'),
)
VOCAB_BLOCK = 1280
GRAD_CHUNKS = (216, 48)
ROW_BLOCK = 528
BLOCK_CALLS = (1, 1, 1, 1)
TOKEN_BLOCK = 1024
POS_BLOCK = 2
OWN_POS_BLOCK = 2
OWN_DEPTH = 4
PLACE_BLOCK = 4


RING = 4
SEMS = ('plane_recv', 'x_recv', 'far_recv', 'plane_send', 'x_send', 'pair_send', 'pair_recv', 'local')
SEMS += ('plane_send_stats', 'pair_send_stats', 'pair_recv_stats', 'local_stats')
HOPS = {k: [hop for hop in itertools.product((0, 1, 2, -1), repeat=2) if sum(map(abs, hop)) == k] for k in range(1, 5)}

SENDS = (('100201,10020-,-00201,-0020-,012210,0122-0,0-2210,0-22-0',
          '-01210,0-1201,1001-0,01010-,1031-0,01310-'),
         ('200201,20020-,022210,0222-0,1-1101,11010-,-12110,1131-0',
          '--1101,-1010-,--2110,1-31-0'),
         ('2-1101,21010-,-22110,1231-0',))


class Exchange:
    def __init__(self, own_ref, stats_ref, all_ref, all_stats_ref, sems, share_rows):
        self.own_ref, self.stats_ref, self.all_ref, self.all_stats_ref = own_ref, stats_ref, all_ref, all_stats_ref
        self.sems = sems
        self.share_rows = share_rows
        self.x = lax.axis_index('tp')
        dp = lax.axis_index('dp')
        self.core = lax.rem(dp, 2)
        self.y = lax.rem(dp // 2, RING)
        self.z = dp // (2 * RING)

    def at(self, dx=0, dy=0, dz=0, other=False):
        x = lax.rem(self.x + dx + RING, RING)
        y = lax.rem(self.y + dy + RING, RING)
        z = lax.rem(self.z + dz + RING, RING)
        core = 1 - self.core if other else self.core
        return (x, (z * RING + y) * 2 + core)

    def pos(self, hop):
        return lax.rem(self.z + hop[1] + RING, RING) * RING + lax.rem(self.y + hop[0] + RING, RING)

    def rows(self, piece):
        kind, start, size = piece
        if kind == 'share':
            start = pl.multiple_of(self.x * self.share_rows, 8)
        return pl.ds(start, size)

    def whole(self, piece):
        return self.all_stats_ref if piece[0] == 'stats' else self.all_ref

    def block(self, piece, hop, rows, first=0, size=4):
        ref = self.whole(piece)
        quarter = ref.shape[3] // 4
        return ref.at[self.core, self.pos(hop), rows, pl.ds(first * quarter, size * quarter)]

    def send(self, src, dst, device, send, recv):
        pltpu.make_async_remote_copy(
            src_ref=src, dst_ref=dst, send_sem=self.sems[send], recv_sem=recv,
            device_id=device, device_id_type=pl.DeviceIdType.MESH).start()

    def barrier(self):
        sem = pltpu.get_barrier_semaphore()
        peers = [self.at(dx=1), self.at(dx=-1), self.at(dx=2), self.at(dy=1), self.at(dy=-1),
                 self.at(dz=1), self.at(dz=-1), self.at(other=True)]
        for peer in peers:
            pl.semaphore_signal(sem, inc=1, device_id=peer, device_id_type=pl.DeviceIdType.MESH)
        pl.semaphore_wait(sem, len(peers))

    def to_pair(self, piece, src, dst):
        end = '_stats' if piece[0] == 'stats' else ''
        self.send(src, dst, self.at(other=True), 'pair_send' + end, self.sems['pair_recv' + end])

    def start_own(self, piece):
        stats = piece[0] == 'stats'
        src = self.stats_ref if stats else self.own_ref
        dst = self.whole(piece).at[self.core, self.pos((0, 0))]
        pltpu.make_async_copy(src, dst, self.sems['local_stats' if stats else 'local']).start()
        self.to_pair(piece, src, dst)

    def round(self, p, piece, k):
        rows, recv = self.rows(piece), self.sems['plane_recv'].at[p, k - 1]
        sent = 'plane_send_stats' if piece[0] == 'stats' else 'plane_send'

        def pass_on(hop, first, size, dy, dz):
            ref = self.block(piece, hop, rows, first, size)
            self.send(ref, ref, self.at(dy=dy, dz=dz), sent, recv)

        if k == 1:
            src = self.stats_ref if piece[0] == 'stats' else self.own_ref.at[rows]
            for dy, dz in HOPS[1]:
                self.send(src, self.block(piece, (0, 0), rows), self.at(dy=dy, dz=dz), sent, recv)
        else:
            for code in ','.join(SENDS[k - 2]).split(','):
                y, z, first, size, dy, dz = ['-0123'.index(c) - 1 for c in code]
                pass_on((y, z), first, size, dy, dz)

    def wait(self, ref, sem):
        pltpu.make_async_copy(ref, ref, sem).wait()

    def finish_round(self, p, piece, k):
        n, rows = len(HOPS[k]), self.rows(piece)
        self.wait(self.whole(piece).at[0, pl.ds(0, n), pl.ds(0, piece[2])], self.sems['plane_recv'].at[p, k - 1])
        for hop in HOPS[k]:
            ref = self.block(piece, hop, rows)
            self.to_pair(piece, ref, ref)
            if piece[0] == 'share':
                for s in (1, -1):
                    self.send(ref, ref, self.at(dx=s), 'x_send', self.sems['x_recv'].at[k - 1])

    def share_of(self, dx):
        x = lax.rem(self.x + dx + RING, RING)
        return pl.ds(pl.multiple_of(x * self.share_rows, 8), self.share_rows)

    def along_x(self, k):
        n, share = len(HOPS[k]), PIECES[0]
        self.wait(self.all_ref.at[0, pl.ds(0, n), pl.ds(0, 2 * self.share_rows)], self.sems['x_recv'].at[k - 1])
        for hop in HOPS[k]:
            for dx, first in ((-1, 0), (1, 2)):
                rows = self.share_of(dx)
                ref = self.block(share, hop, rows, first, 2)
                self.send(ref, ref, self.at(dx=-dx), 'x_send', self.sems['far_recv'].at[k - 1])
                ref = self.block(share, hop, rows)
                self.to_pair(share, ref, ref)

    def finish_x(self, k):
        n, share, rows = len(HOPS[k]), PIECES[0], self.share_of(2)
        self.wait(self.all_ref.at[0, pl.ds(0, n), pl.ds(0, self.share_rows)], self.sems['far_recv'].at[k - 1])
        for hop in HOPS[k]:
            ref = self.block(share, hop, rows)
            self.to_pair(share, ref, ref)

    def finish(self, pieces):
        others = pl.ds(0, RING * RING - 1)
        total = sum(size for kind, _, size in pieces if kind != 'stats')
        for end, ref in (('', self.all_ref), ('_stats', self.all_stats_ref)):
            self.wait(ref.at[0], self.sems['pair_recv' + end])
            self.wait(ref.at[0], self.sems['pair_send' + end])
            self.wait(ref.at[0, 0], self.sems['local' + end])
        self.wait(self.all_ref.at[0, others, pl.ds(0, total)], self.sems['plane_send'])
        self.wait(self.all_stats_ref.at[0, others], self.sems['plane_send_stats'])
        self.wait(self.all_ref.at[0, others, pl.ds(0, 3 * self.share_rows)], self.sems['x_send'])


def exchange_kernel(plan, pieces, share_rows, vocab, inv_n, h_ref, own_ref, emb_ref, ids_ref, tgt_ref,
                    all_ref, all_stats_ref, grad_ref, stats_out_ref,
                    logits_ref, m_ref, s_ref, t_ref, col_ref, stats_ref, part_ref, part_recv, part_send, *sem_refs):
    step = pl.program_id(0)
    n_tiles, rows, width = logits_ref.shape
    ex = Exchange(own_ref, stats_ref, all_ref, all_stats_ref, dict(zip(SEMS, sem_refs)), share_rows)

    def run(event):
        kind, *nums = event
        nums = [int(v) for v in nums]
        if kind == 's':
            ex.round(nums[0], pieces[nums[0]], 1)
        elif kind == 'r':
            p, k = nums
            ex.finish_round(p, pieces[p], k)
            if k < 4:
                ex.round(p, pieces[p], k + 1)
        elif kind == 'x':
            ex.along_x(nums[0])
        else:
            ex.finish_x(nums[0])

    for i, groups in enumerate(plan):
        events = [event for group in groups for event in group.split(',')]
        if events:
            @pl.when(step == i)
            def _(i=i, events=events):
                if i == 0:
                    ex.barrier()
                    ex.start_own(pieces[0])
                for event in events:
                    run(event)
                if i == len(plan) - 1:
                    ex.finish(pieces)

    @pl.when(step == 0)
    def _():
        m_ref[...] = jnp.full_like(m_ref, -jnp.inf)
        s_ref[...] = jnp.zeros_like(s_ref)
        t_ref[...] = jnp.zeros_like(t_ref)
        grad_ref[...] = jnp.zeros_like(grad_ref)

    @pl.when(step < n_tiles)
    def _():
        logits = lax.dot_general(h_ref[...], emb_ref[...], NT, preferred_element_type=jnp.float32)
        logits_ref[step] = logits
        lane = lax.broadcasted_iota(jnp.int32, (rows, LANES), 1)
        tgt_sum = t_ref[...]
        parts = []
        for j in range(width // LANES):
            ids = lane + (step * width + j * LANES)
            part = jnp.where(ids < vocab, logits[:, j * LANES:(j + 1) * LANES], -jnp.inf)
            tgt_sum += jnp.where(ids == ids_ref[...], part, 0.0)
            parts.append(part)
        t_ref[...] = tgt_sum
        m_old = m_ref[...]
        m_new = functools.reduce(jnp.maximum, parts, m_old)
        floor = jnp.where(m_new == -jnp.inf, 0.0, m_new)
        s_new = s_ref[...] * jnp.exp(m_old - floor)
        for part in parts:
            s_new += jnp.exp(part - floor)
        m_ref[...] = m_new
        s_ref[...] = s_new

    @pl.when(step == n_tiles)
    def _():
        m_col = jnp.max(m_ref[...], axis=1, keepdims=True)
        s_col = jnp.sum(s_ref[...] * jnp.exp(m_ref[...] - m_col), axis=1, keepdims=True)
        t_col = jnp.sum(t_ref[...], axis=1, keepdims=True)
        lane = lax.broadcasted_iota(jnp.int32, (rows, LANES), 1)
        cols = jnp.where(lane == 0, m_col, jnp.where(lane == 1, s_col, jnp.where(lane == 2, t_col, 0.0)))
        part_ref[ex.x] = cols.T[:8]
        for dx in (1, 2, 3):
            dst = part_ref.at[ex.x]
            pltpu.make_async_remote_copy(
                src_ref=dst, dst_ref=dst, send_sem=part_send, recv_sem=part_recv,
                device_id=ex.at(dx=dx), device_id_type=pl.DeviceIdType.MESH).start()
        ex.wait(part_ref.at[pl.ds(0, 3)], part_recv)
        ex.wait(part_ref.at[pl.ds(0, 3)], part_send)
        m_row = functools.reduce(jnp.maximum, [part_ref[i, 0:1] for i in range(RING)])
        s_row = sum(part_ref[i, 1:2] * jnp.exp(part_ref[i, 0:1] - m_row) for i in range(RING))
        t_row = sum(part_ref[i, 2:3] for i in range(RING))
        sub = lax.broadcasted_iota(jnp.int32, (8, rows), 0)
        values = (m_row, inv_n / s_row, tgt_ref[...], s_row, t_row)
        final = jnp.zeros((8, rows), jnp.float32)
        for i, value in enumerate(values):
            final = jnp.where(sub == i, value, final)
        stats_out_ref[...] = final
        stats_ref[...] = jnp.zeros_like(stats_ref)
        stats_ref[:, :rows] = final
        col_ref[...] = jnp.concatenate([final, jnp.zeros((LANES - 8, rows), jnp.float32)]).T
        ex.start_own(pieces[-1])

    def add_grad(masked):
        tile = step - n_tiles
        ids = lax.broadcasted_iota(jnp.int32, (rows, width), 1) + tile * width
        grad = jnp.exp(logits_ref[tile] - col_ref[:, 0:1]) * col_ref[:, 1:2]
        grad -= jnp.where(ids == ids_ref[...], inv_n, 0.0)
        if masked:
            grad = jnp.where(ids < vocab, grad, 0.0)
        grad = grad.astype(jnp.bfloat16)
        n_cols = grad_ref.shape[1] // 4

        @pl.loop(0, 4)
        def _(j):
            cols = pl.ds(pl.multiple_of(j * n_cols, LANES), n_cols)
            emb = emb_ref[:, cols]
            if masked:
                emb_ids = lax.broadcasted_iota(jnp.int32, emb.shape, 0) + tile * width
                emb = jnp.where(emb_ids < vocab, emb.astype(jnp.float32), 0.0).astype(emb.dtype)
            grad_ref[:, cols] += jnp.dot(grad, emb, preferred_element_type=jnp.float32)

    pl.when(jnp.logical_and(step >= n_tiles, step < 2 * n_tiles - 1))(lambda: add_grad(False))
    pl.when(step == 2 * n_tiles - 1)(lambda: add_grad(True))


def exchange_tokens(h_act, h_wide, emb, local_ids, tgt_row, inv_n, n_dp):
    rows, width = h_act.shape
    vocab = emb.shape[0]
    n_tiles = pl.cdiv(vocab, VOCAB_BLOCK)
    n_steps = 2 * n_tiles + 1
    plan = PLAN if len(PLAN) == n_steps else PLAN[:-1] + ((),) * (n_steps - len(PLAN)) + PLAN[-1:]
    dma = pltpu.SemaphoreType.DMA
    emb_tile = lambda i: (jnp.where(i < n_tiles, i, jnp.minimum(i - n_tiles, n_tiles - 1)), 0)
    whole = pl.BlockSpec(memory_space=pltpu.VMEM)
    return pl.pallas_call(
        functools.partial(exchange_kernel, plan, PIECES, SHARE_ROWS, vocab, inv_n),
        out_shape=(jax.ShapeDtypeStruct((2, n_dp // 2, rows, width), jnp.float32),
                   jax.ShapeDtypeStruct((2, n_dp // 2, 8, 4 * LANES), jnp.float32),
                   jax.ShapeDtypeStruct((rows, width), jnp.float32),
                   jax.ShapeDtypeStruct((8, rows), jnp.float32)),
        grid=(n_steps,),
        in_specs=[whole, whole, pl.BlockSpec((VOCAB_BLOCK, width), emb_tile), whole, whole],
        out_specs=(pl.BlockSpec(memory_space=pl.ANY), pl.BlockSpec(memory_space=pl.ANY), whole, whole),
        scratch_shapes=[pltpu.VMEM((n_tiles, rows, VOCAB_BLOCK), jnp.float32)]
                       + [pltpu.VMEM((rows, LANES), jnp.float32)] * 4
                       + [pltpu.VMEM((8, 4 * LANES), jnp.float32), pltpu.VMEM((RING, 8, rows), jnp.float32)]
                       + [dma, dma, dma((len(PIECES), 4)), dma((4,)), dma((4,))] + [dma] * (len(SEMS) - 3),
        compiler_params=pltpu.CompilerParams(
            vmem_limit_bytes=VMEM_LIMIT, collective_id=0, has_side_effects=True),
        cost_estimate=pl.CostEstimate(
            flops=60 * rows * vocab * width, bytes_accessed=vocab * 4 * width, transcendentals=2 * rows * vocab),
        name="exchange_tokens",
    )(h_act, h_wide, emb, local_ids, tgt_row)


def row_grads(inv_n, emb, row_ids, h_blk, stats):
    logits = lax.dot_general(emb, h_blk, NT, preferred_element_type=jnp.float32)
    prob = jnp.exp(logits - stats[0:1]) * stats[1:2]
    grad = prob - jnp.where(row_ids == stats[2:3], inv_n, 0.0)
    return jnp.dot(grad.astype(jnp.bfloat16), h_blk, preferred_element_type=jnp.float32)


def id_column(n_rows, first):
    return (lax.broadcasted_iota(jnp.int32, (n_rows, 1), 0) + first).astype(jnp.float32)


def load_tokens(all_ref, all_stats_ref):
    _, blocks, rows, width = all_ref.shape
    h_blk = all_ref[0].reshape(blocks * rows, width).astype(jnp.bfloat16)
    return h_blk, jnp.concatenate([all_stats_ref[0, i, :, :rows] for i in range(blocks)], axis=1)


def token_specs(gathered, pos_block):
    return [pl.BlockSpec((1, pos_block) + arr.shape[2:],
                         lambda i, where: (i * pos_block // arr.shape[1], lax.rem(i, arr.shape[1] // pos_block), 0, 0))
            for arr in gathered]


def own_rows_kernel(inv_n, bases, where, emb0_ref, emb1_ref, all_ref, all_stats_ref, own0_ref, own1_ref,
                    emb_ref, acc_ref, stage_ref, sem):
    n0, n1 = emb0_ref.shape[0], emb1_ref.shape[0]
    step, n_steps = pl.program_id(0), pl.num_programs(0)
    depth, n_pos = stage_ref.shape[0], stage_ref.shape[1]
    per_core = all_ref.shape[1] // n_pos

    def load(i):
        src = all_ref.at[i // per_core, pl.ds(lax.rem(i, per_core) * n_pos, n_pos)]
        slot = lax.rem(i, depth)
        return pltpu.make_async_copy(src, stage_ref.at[slot], sem.at[slot])

    @pl.when(step == 0)
    def _():
        for i in range(depth - 1):
            load(i).start()

    load(step).wait()

    @pl.when(step + depth - 1 < n_steps)
    def _():
        load(step + depth - 1).start()


    @pl.when(pl.program_id(0) == 0)
    def _():
        emb_ref[:n0] = emb0_ref[...]
        emb_ref[n0:] = emb1_ref[...]
        acc_ref[...] = jnp.zeros_like(acc_ref)

    first0, first1 = [where[1] + base + where[0] * n for base, n in zip(bases, (n0, n1))]
    row = lax.broadcasted_iota(jnp.int32, (n0 + n1, 1), 0)
    row_ids = (row + jnp.where(row < n0, first0, first1 - n0)).astype(jnp.float32)
    h_blk, stats = load_tokens(stage_ref.at[pl.ds(lax.rem(step, depth), 1)], all_stats_ref)
    acc_ref[...] += row_grads(inv_n, emb_ref[...], row_ids, h_blk, stats)

    @pl.when(pl.program_id(0) == pl.num_programs(0) - 1)
    def _():
        own0_ref[...] = acc_ref[:n0]
        own1_ref[:n1] = acc_ref[n0:]
        own1_ref[n1:] = jnp.zeros_like(own1_ref[n1:])


def own_rows(emb, gathered, where, inv_n, n_dp):
    width = emb.shape[1]
    n_tok = gathered[0].size // width
    n0, n1 = GRAD_CHUNKS
    bases = (0, n_dp * n0)
    emb_spec = lambda base, n: pl.BlockSpec((n, width), lambda i, where: (base // n + where[0], 0))
    whole = lambda n: pl.BlockSpec((n, width), lambda i, where: (0, 0))
    return pl.pallas_call(
        functools.partial(own_rows_kernel, inv_n, bases),
        out_shape=(jax.ShapeDtypeStruct((n0, width), jnp.float32), jax.ShapeDtypeStruct((n1 + 8, width), jnp.float32)),
        grid_spec=pltpu.PrefetchScalarGridSpec(
            num_scalar_prefetch=1,
            grid=(gathered[0].shape[0] * gathered[0].shape[1] // OWN_POS_BLOCK,),
            in_specs=[emb_spec(bases[0], n0), emb_spec(bases[1], n1),
                      pl.BlockSpec(memory_space=pl.ANY), token_specs(gathered, OWN_POS_BLOCK)[1]],
            out_specs=(whole(n0), whole(n1 + 8)),
            scratch_shapes=[pltpu.VMEM((n0 + n1, width), jnp.bfloat16), pltpu.VMEM((n0 + n1, width), jnp.float32),
                            pltpu.VMEM((OWN_DEPTH, OWN_POS_BLOCK) + gathered[0].shape[2:], jnp.float32),
                            pltpu.SemaphoreType.DMA((OWN_DEPTH,))]),
        compiler_params=pltpu.CompilerParams(vmem_limit_bytes=VMEM_LIMIT),
        cost_estimate=pl.CostEstimate(
            flops=4 * (n0 + n1) * n_tok * width, bytes_accessed=n_tok * width * 4, transcendentals=(n0 + n1) * n_tok),
        name="own_rows",
    )(where, emb, emb, *gathered)


def first_block_kernel(inv_n, first, where, emb_ref, all_ref, all_stats_ref, out_ref, copy_ref, h_ref, stats_ref):
    step, last = pl.program_id(0), pl.num_programs(0) - 1

    @pl.when(step == 0)
    def _():
        out_ref[...] = jnp.zeros_like(out_ref)

    h_blk, stats = load_tokens(all_ref, all_stats_ref)
    h_ref[...] = h_blk
    stats_ref[...] = stats
    n_rows = emb_ref.shape[0]
    row_ids = id_column(n_rows, where[1] + (where[2] + first) * n_rows)
    out_ref[...] += row_grads(inv_n, emb_ref[...], row_ids, h_blk, stats)

    @pl.when(step == last)
    def _():
        copy_ref[...] = out_ref[...]


def first_block(emb, gathered, where, inv_n, first):
    vocab, width = emb.shape
    n_tok = gathered[0].size // width
    per_step = POS_BLOCK * gathered[0].shape[2]
    row_spec = pl.BlockSpec((ROW_BLOCK, width), lambda i, where: (first + where[2], 0))
    return pl.pallas_call(
        functools.partial(first_block_kernel, inv_n, first),
        out_shape=(jax.ShapeDtypeStruct((vocab, width), jnp.float32),
                   jax.ShapeDtypeStruct((ROW_BLOCK, width), jnp.float32),
                   jax.ShapeDtypeStruct((n_tok, width), jnp.bfloat16),
                   jax.ShapeDtypeStruct((8, n_tok), jnp.float32)),
        grid_spec=pltpu.PrefetchScalarGridSpec(
            num_scalar_prefetch=1,
            grid=(n_tok // per_step,),
            in_specs=[row_spec] + token_specs(gathered, POS_BLOCK),
            out_specs=(row_spec, pl.BlockSpec((ROW_BLOCK, width), lambda i, where: (0, 0)),
                       pl.BlockSpec((per_step, width), lambda i, where: (i, 0)),
                       pl.BlockSpec((8, per_step), lambda i, where: (0, i)))),
        compiler_params=pltpu.CompilerParams(vmem_limit_bytes=VMEM_LIMIT),
        cost_estimate=pl.CostEstimate(
            flops=4 * ROW_BLOCK * n_tok * width, bytes_accessed=n_tok * width * 6, transcendentals=ROW_BLOCK * n_tok),
        name="first_block",
    )(where, emb, *gathered)


class Placing:
    def __init__(self, out_ref, got_ref, recv_refs, recv_rows, n_steps, stages, sems):
        self.out_ref, self.got_ref, self.recv_refs, self.recv_rows = out_ref, got_ref, recv_refs, recv_rows
        self.n_steps, self.stages, self.sems = n_steps, stages, sems
        self.per_step = got_ref.shape[0] // n_steps
        self.n_got = stages[0].shape[2]
        self.n_recv = stages[1].shape[1]
        self.parts = recv_refs[0].shape[0] // self.n_recv

    def copies(self, step, slot, store):
        sem = self.sems.at[1 if store else 0, slot]
        for j in range(self.per_step):
            i = step * self.per_step + j
            stage = self.stages[0].at[slot, j]
            if store:
                yield pltpu.make_async_copy(stage, self.out_ref.at[pl.ds(pl.multiple_of(i * self.n_got, 8), self.n_got)], sem)
            else:
                yield pltpu.make_async_copy(self.got_ref.at[i, pl.ds(0, self.n_got)], stage, sem)

    def recv_copy(self, step, slot, store, k):
        sem = self.sems.at[3 if store else 2, slot]
        part = (step - k * self.parts) * self.n_recv
        stage = self.stages[1].at[slot]
        if store:
            row = pl.multiple_of(self.recv_rows[k] + part, 8)
            return pltpu.make_async_copy(stage, self.out_ref.at[pl.ds(row, self.n_recv)], sem)
        return pltpu.make_async_copy(self.recv_refs[k].at[pl.ds(pl.multiple_of(part, 8), self.n_recv)], stage, sem)

    def each(self, step, store, act):
        slot = lax.rem(step, 2)
        for copy in self.copies(step, slot, store):
            act(copy)
        for k in range(len(self.recv_refs)):
            @pl.when(jnp.logical_and(step >= k * self.parts, step < (k + 1) * self.parts))
            def _(k=k):
                act(self.recv_copy(step, slot, store, k))

    def before(self, step):
        @pl.when(step >= 1)
        def _():
            self.each(step - 1, False, lambda c: c.wait())
            self.each(step - 1, True, lambda c: c.start())

        @pl.when(step >= 2)
        def _():
            self.each(step - 2, True, lambda c: c.wait())

        self.each(step, False, lambda c: c.start())

    def after(self, step):
        @pl.when(step == self.n_steps - 1)
        def _():
            self.each(step, False, lambda c: c.wait())
            self.each(step, True, lambda c: c.start())
            self.each(step - 1, True, lambda c: c.wait())
            self.each(step, True, lambda c: c.wait())


def grad_rows_kernel(inv_n, first, n_steps, recv_firsts, where, emb_ref, h_ref, stats_ref, *refs):
    i, t = pl.program_id(0), pl.program_id(1)
    n_ref = 2 + len(recv_firsts) if recv_firsts else 1
    out_in_ref, acc_ref, copy_ref = refs[0], refs[n_ref], refs[n_ref + 1]
    n_rows = emb_ref.shape[0]
    placing = None
    if recv_firsts:
        rows = [(where[3] + block) * n_rows for block in recv_firsts]
        placing = Placing(out_in_ref, refs[1], refs[2:n_ref], rows, n_steps, refs[n_ref + 2:n_ref + 4], refs[n_ref + 4])
        placing.before(i * pl.num_programs(1) + t)

    @pl.when(t == 0)
    def _():
        acc_ref[...] = jnp.zeros_like(acc_ref)

    row_ids = id_column(n_rows, where[1] + (where[2] + first + i) * n_rows)
    acc_ref[...] += row_grads(inv_n, emb_ref[...], row_ids, h_ref[...], stats_ref[...])

    @pl.when(t == pl.num_programs(1) - 1)
    def _():
        copy_ref[...] = acc_ref[...]

    if placing:
        placing.after(i * pl.num_programs(1) + t)


def grad_rows(emb, h_all, stats, where, out, inv_n, first, n_blocks, got=None, n_got=0, recvs=(), recv_firsts=()):
    vocab, width = emb.shape
    n_tok = h_all.shape[0]
    tok_block = min(TOKEN_BLOCK, n_tok)
    n_steps = n_blocks * (n_tok // tok_block)
    row_spec = pl.BlockSpec((ROW_BLOCK, width), lambda i, t, where: (i + first + where[2], 0))
    anywhere = pl.BlockSpec(memory_space=pl.ANY)
    in_specs = [row_spec, pl.BlockSpec((tok_block, width), lambda i, t, where: (t, 0)),
                pl.BlockSpec((8, tok_block), lambda i, t, where: (0, t)), anywhere]
    args, scratch = [emb, h_all, stats, out], []
    if recvs:
        args += [got, *recvs]
        in_specs += [anywhere] * (1 + len(recvs))
        part = ROW_BLOCK * len(recvs) // n_steps
        part = next(n for n in range(part // 8 * 8 or 8, ROW_BLOCK + 1, 8) if ROW_BLOCK % n == 0 and n * n_steps >= ROW_BLOCK * len(recvs))
        scratch = [pltpu.VMEM((2, got.shape[0] // n_steps, n_got, width), jnp.float32),
                   pltpu.VMEM((2, part, width), jnp.float32), pltpu.SemaphoreType.DMA((4, 2))]
    rows = n_blocks * ROW_BLOCK
    return pl.pallas_call(
        functools.partial(grad_rows_kernel, inv_n, first, n_steps, tuple(recv_firsts)),
        out_shape=(jax.ShapeDtypeStruct((vocab, width), jnp.float32), jax.ShapeDtypeStruct((rows, width), jnp.float32)),
        grid_spec=pltpu.PrefetchScalarGridSpec(
            num_scalar_prefetch=1,
            grid=(n_blocks, n_tok // tok_block),
            in_specs=in_specs,
            out_specs=(row_spec, pl.BlockSpec((ROW_BLOCK, width), lambda i, t, where: (i, 0))),
            scratch_shapes=scratch),
        input_output_aliases={4: 0},
        compiler_params=pltpu.CompilerParams(vmem_limit_bytes=VMEM_LIMIT),
        cost_estimate=pl.CostEstimate(
            flops=4 * rows * n_tok * width,
            bytes_accessed=rows * width * 6 + n_blocks * n_tok * width * 2,
            transcendentals=rows * n_tok),
        name="grad_rows",
    )(where, *args)


def place_kernel(where, src_ref, prev_ref, dst_ref, *sum_refs):
    del where, prev_ref
    n_dev, n_rows = src_ref.shape[0], dst_ref.shape[0] // src_ref.shape[0]
    for i in range(n_dev):
        dst_ref[i * n_rows:(i + 1) * n_rows] = src_ref[i, :n_rows]
    for sum_ref in sum_refs:
        @pl.when(pl.program_id(0) == 0)
        def _(sum_ref=sum_ref):
            sum_ref[...] = jnp.zeros_like(sum_ref)

        sum_ref[...] += sum(src_ref[i, n_rows:] for i in range(n_dev))


def place_rows(src, n_rows, out, where, first_block, per_block, with_sums=False):
    n_src, n_in, width = src.shape
    placed = pl.pallas_call(
        place_kernel,
        out_shape=[jax.ShapeDtypeStruct(out.shape, out.dtype)]
                  + [jax.ShapeDtypeStruct((n_in - n_rows, width), out.dtype)] * with_sums,
        grid_spec=pltpu.PrefetchScalarGridSpec(
            num_scalar_prefetch=1,
            grid=(n_src // per_block,),
            in_specs=[pl.BlockSpec((per_block, n_in, width), lambda i, where: (i, 0, 0)),
                      pl.BlockSpec(memory_space=pl.ANY)],
            out_specs=[pl.BlockSpec((per_block * n_rows, width), lambda i, where: (i + first_block + where[3], 0))]
                      + [pl.BlockSpec((n_in - n_rows, width), lambda i, where: (0, 0))] * with_sums),
        input_output_aliases={2: 0},
        compiler_params=pltpu.CompilerParams(vmem_limit_bytes=VMEM_LIMIT),
        cost_estimate=pl.CostEstimate(flops=src.size * 80, bytes_accessed=src.size * 8, transcendentals=0),
        name="place_rows",
    )(where, src, out)
    return placed if with_sums else placed[0]


def shifts(n_tp):
    return [[(i, (i + shift) % n_tp) for i in range(n_tp)] for shift in range(1, n_tp)]


def send_blocks(part, n_tp, tp_idx):
    blocks = part.reshape(n_tp, part.shape[0] // n_tp, part.shape[1])
    pick = lambda i: lax.dynamic_index_in_dim(blocks, i % n_tp, 0, keepdims=False)
    return [pick(tp_idx)] + [lax.ppermute(pick(tp_idx + 1 + d), 'tp', perm) for d, perm in enumerate(shifts(n_tp))]


def send_total(blocks, n_tp):
    total = functools.reduce(jnp.add, blocks)
    return [total] + [lax.ppermute(total, 'tp', perm) for perm in shifts(n_tp)]


def join_totals(totals, n_tp, tp_idx):
    whole = jnp.zeros((n_tp,) + totals[0].shape, totals[0].dtype)
    for shift, total in enumerate(totals):
        whole = lax.dynamic_update_index_in_dim(whole, total, (tp_idx + n_tp - shift) % n_tp, 0)
    return whole.reshape(-1, totals[0].shape[1])


def solution(mesh):
    n_tp, n_dp = mesh.shape['tp'], mesh.shape['dp']

    def program(hidden, residual, targets, embedding, norm_w):
        inv_n = 1.0 / (hidden.shape[0] * hidden.shape[1])

        def local_part(hid_loc, res_loc, tgt_loc, emb_loc, norm_vec):
            n_batch, n_seq, d_model = hid_loc.shape
            n_rows = n_batch * n_seq
            vocab_loc = emb_loc.shape[0]
            tp_idx, dp_idx = lax.axis_index('tp'), lax.axis_index('dp')
            resid = (res_loc + hid_loc.astype(jnp.float32)).reshape(n_rows, d_model)
            tgt_rows = tgt_loc.reshape(n_rows)
            inv_rms = lax.rsqrt(jnp.mean(resid * resid, axis=-1, keepdims=True) + NORM_EPS)
            scaled_r = resid * inv_rms
            h_wide = lax.reduce_precision(scaled_r * norm_vec, exponent_bits=8, mantissa_bits=7)
            h_act = h_wide.astype(jnp.bfloat16)
            local_ids = (tgt_rows - tp_idx * vocab_loc)[:, None]
            local_ids = jnp.where(local_ids < vocab_loc, local_ids, -1)
            tgt_row = tgt_rows.astype(jnp.float32)[None]
            *gathered, grad_h, stats = exchange_tokens(h_act, h_wide, emb_loc, local_ids, tgt_row, inv_n, n_dp)
            loss_part = jnp.sum(stats[0] + jnp.log(stats[3]) - stats[4]) * inv_n

            per_core = sum(BLOCK_CALLS)
            core = dp_idx % 2
            where = jnp.stack([dp_idx, tp_idx * vocab_loc, core * per_core, (1 - core) * per_core]).astype(jnp.int32)
            own0, own1 = own_rows(emb_loc, gathered, where, inv_n, n_dp)
            got0 = lax.all_gather(own0, 'dp')
            gathered, grad_h, own0 = lax.optimization_barrier((gathered, grad_h, own0))
            grad_h = send_blocks(grad_h, n_tp, tp_idx)

            first = n_dp * sum(GRAD_CHUNKS) // ROW_BLOCK
            pair = [(i, i ^ 1) for i in range(n_dp)]
            out, copied, h_all, all_stats = first_block(emb_loc, gathered, where, inv_n, first)
            recvs, recv_firsts, late, block = [], [], [], first
            for c, n_blocks in enumerate(BLOCK_CALLS):
                final = c == len(BLOCK_CALLS) - 1
                if c:
                    extra = (got0, GRAD_CHUNKS[0], recvs, recv_firsts) if final else ()
                    out, copied = grad_rows(emb_loc, h_all, all_stats, where, out, inv_n, block, n_blocks, *extra)
                if c < 2:
                    grad_h, out = lax.optimization_barrier((grad_h, out))
                    grad_h = join_totals(grad_h, n_tp, tp_idx) if c else send_total(grad_h, n_tp)
                recv = lax.ppermute(copied, 'dp', pair)
                if c < len(BLOCK_CALLS) - 2:
                    recvs.append(recv)
                    recv_firsts.append(block)
                else:
                    late.append((recv, block))
                block += n_blocks
                if c == 1:
                    grad_scaled = grad_h * norm_vec
                    grad_r = inv_rms * (grad_scaled - scaled_r * jnp.mean(grad_scaled * scaled_r, axis=-1, keepdims=True))
                    grad_w = jnp.sum(grad_h * scaled_r, axis=0)
                    own1 = own1.at[-8].set(grad_w).at[-7, 0].set(loss_part)
                    got1 = lax.all_gather(own1, 'dp')

            n_own = GRAD_CHUNKS[1]
            n_place = PLACE_BLOCK * n_own
            (recv, block), (last_recv, last_block) = late
            for part, start in ((recv, block), (last_recv, last_block)):
                out = place_rows(part.reshape(-1, ROW_BLOCK, d_model), ROW_BLOCK, out, where, start, 1)
            out, sums = place_rows(got1, n_own, out, jnp.zeros_like(where), n_dp * GRAD_CHUNKS[0] // n_place, PLACE_BLOCK, True)
            return sums[1, 0], grad_r.reshape(n_batch, n_seq, d_model), out, sums[0]

        sharded = jax.shard_map(
            local_part, mesh=mesh,
            in_specs=(P('dp', None, None), P('dp', None, None), P('dp', None), P('tp', None), P(None)),
            out_specs=(P(), P('dp', None, None), P('tp', None), P(None)),
            check_vma=False)
        return sharded(hidden, residual, targets, embedding, norm_w)

    return program
```

```python
import functools
import itertools

import jax
import jax.numpy as jnp
from jax import lax
from jax.experimental import pallas as pl
from jax.experimental.pallas import tpu as pltpu
from jax.sharding import PartitionSpec as P


NORM_EPS = 1e-5
LANES = 128
VMEM_LIMIT = 60 << 20
NT = (((1,), (1,)), ((), ()))
SHARE_ROWS = 24
DIRECT_ROWS = 40
PIECES = (('share', 0, SHARE_ROWS),)
PIECES += tuple(('direct', 4 * SHARE_ROWS + i * DIRECT_ROWS, DIRECT_ROWS) for i in range(4))
PIECES += (('stats', 0, 8),)
PLAN = (
    ('s0,s1',),
    (),
    (),
    ('s2',),
    ('r01',),
    (),
    (),
    ('r11',),
    (),
    (),
    ('r21',),
    ('s5',),
    (),
    ('r02,x1',),
    (),
    (),
    (),
    (),
    ('r12',),
    (),
    ('r22,r51,r03,x2,s3,r13,f1,r23,r52,r04,s4,r31,r14,r24', 'r53,x3,r41,f2,r32,r54,x4,f3,r42,f4,r33,r43,r34,r44'),
)
VOCAB_BLOCK = 1280
GRAD_CHUNKS = (192, 64)
ROW_BLOCK = 576
BLOCK_CALLS = (2, 1, 1)
TOKEN_BLOCK = 1024
POS_BLOCK = 2
OWN_POS_BLOCK = 2
OWN_DEPTH = 4
PLACE_BLOCK = 4


RING = 4
SEMS = ('plane_recv', 'x_recv', 'far_recv', 'plane_send', 'x_send', 'pair_send', 'pair_recv', 'local')
SEMS += ('plane_send_stats', 'pair_send_stats', 'pair_recv_stats', 'local_stats')
HOPS = {k: [hop for hop in itertools.product((0, 1, 2, -1), repeat=2) if sum(map(abs, hop)) == k] for k in range(1, 5)}

SENDS = (('100201,10020-,-00201,-0020-,012210,0122-0,0-2210,0-22-0',
          '-01210,0-1201,1001-0,01010-,1031-0,01310-'),
         ('200201,20020-,022210,0222-0,1-1101,11010-,-12110,1131-0',
          '--1101,-1010-,--2110,1-31-0'),
         ('2-1101,21010-,-22110,1231-0',))


class Exchange:
    def __init__(self, own_ref, stats_ref, all_ref, all_stats_ref, sems, share_rows):
        self.own_ref, self.stats_ref, self.all_ref, self.all_stats_ref = own_ref, stats_ref, all_ref, all_stats_ref
        self.sems = sems
        self.share_rows = share_rows
        self.x = lax.axis_index('tp')
        dp = lax.axis_index('dp')
        self.core = lax.rem(dp, 2)
        self.y = lax.rem(dp // 2, RING)
        self.z = dp // (2 * RING)

    def at(self, dx=0, dy=0, dz=0, other=False):
        x = lax.rem(self.x + dx + RING, RING)
        y = lax.rem(self.y + dy + RING, RING)
        z = lax.rem(self.z + dz + RING, RING)
        core = 1 - self.core if other else self.core
        return (x, (z * RING + y) * 2 + core)

    def pos(self, hop):
        return lax.rem(self.z + hop[1] + RING, RING) * RING + lax.rem(self.y + hop[0] + RING, RING)

    def rows(self, piece):
        kind, start, size = piece
        if kind == 'share':
            start = pl.multiple_of(self.x * self.share_rows, 8)
        return pl.ds(start, size)

    def whole(self, piece):
        return self.all_stats_ref if piece[0] == 'stats' else self.all_ref

    def block(self, piece, hop, rows, first=0, size=4):
        ref = self.whole(piece)
        quarter = ref.shape[3] // 4
        return ref.at[self.core, self.pos(hop), rows, pl.ds(first * quarter, size * quarter)]

    def send(self, src, dst, device, send, recv):
        pltpu.make_async_remote_copy(
            src_ref=src, dst_ref=dst, send_sem=self.sems[send], recv_sem=recv,
            device_id=device, device_id_type=pl.DeviceIdType.MESH).start()

    def barrier(self):
        sem = pltpu.get_barrier_semaphore()
        peers = [self.at(dx=1), self.at(dx=-1), self.at(dx=2), self.at(dy=1), self.at(dy=-1),
                 self.at(dz=1), self.at(dz=-1), self.at(other=True)]
        for peer in peers:
            pl.semaphore_signal(sem, inc=1, device_id=peer, device_id_type=pl.DeviceIdType.MESH)
        pl.semaphore_wait(sem, len(peers))

    def to_pair(self, piece, src, dst):
        end = '_stats' if piece[0] == 'stats' else ''
        self.send(src, dst, self.at(other=True), 'pair_send' + end, self.sems['pair_recv' + end])

    def start_own(self, piece):
        stats = piece[0] == 'stats'
        src = self.stats_ref if stats else self.own_ref
        dst = self.whole(piece).at[self.core, self.pos((0, 0))]
        pltpu.make_async_copy(src, dst, self.sems['local_stats' if stats else 'local']).start()
        self.to_pair(piece, src, dst)

    def round(self, p, piece, k):
        rows, recv = self.rows(piece), self.sems['plane_recv'].at[p, k - 1]
        sent = 'plane_send_stats' if piece[0] == 'stats' else 'plane_send'

        def pass_on(hop, first, size, dy, dz):
            ref = self.block(piece, hop, rows, first, size)
            self.send(ref, ref, self.at(dy=dy, dz=dz), sent, recv)

        if k == 1:
            src = self.stats_ref if piece[0] == 'stats' else self.own_ref.at[rows]
            for dy, dz in HOPS[1]:
                self.send(src, self.block(piece, (0, 0), rows), self.at(dy=dy, dz=dz), sent, recv)
        else:
            for code in ','.join(SENDS[k - 2]).split(','):
                y, z, first, size, dy, dz = ['-0123'.index(c) - 1 for c in code]
                pass_on((y, z), first, size, dy, dz)

    def wait(self, ref, sem):
        pltpu.make_async_copy(ref, ref, sem).wait()

    def wait_round(self, p, piece, k):
        blocks = self.whole(piece).at[0, pl.ds(0, len(HOPS[k])), pl.ds(0, piece[2])]
        self.wait(blocks, self.sems['plane_recv'].at[p, k - 1])

    def forward(self, piece, k):
        rows = self.rows(piece)
        for hop in HOPS[k]:
            ref = self.block(piece, hop, rows)
            if piece[0] == 'share':
                for s in (1, -1):
                    self.send(ref, ref, self.at(dx=s), 'x_send', self.sems['x_recv'].at[k - 1])
            self.to_pair(piece, ref, ref)

    def share_of(self, dx):
        x = lax.rem(self.x + dx + RING, RING)
        return pl.ds(pl.multiple_of(x * self.share_rows, 8), self.share_rows)

    def along_x(self, k):
        n, share = len(HOPS[k]), PIECES[0]
        self.wait(self.all_ref.at[0, pl.ds(0, n), pl.ds(0, 2 * self.share_rows)], self.sems['x_recv'].at[k - 1])
        for hop in HOPS[k]:
            for dx, first in ((-1, 0), (1, 2)):
                rows = self.share_of(dx)
                ref = self.block(share, hop, rows, first, 2)
                self.send(ref, ref, self.at(dx=-dx), 'x_send', self.sems['far_recv'].at[k - 1])
                ref = self.block(share, hop, rows)
                self.to_pair(share, ref, ref)

    def finish_x(self, k):
        n, share, rows = len(HOPS[k]), PIECES[0], self.share_of(2)
        self.wait(self.all_ref.at[0, pl.ds(0, n), pl.ds(0, self.share_rows)], self.sems['far_recv'].at[k - 1])
        for hop in HOPS[k]:
            ref = self.block(share, hop, rows)
            self.to_pair(share, ref, ref)

    def finish(self, pieces):
        others = pl.ds(0, RING * RING - 1)
        total = sum(size for kind, _, size in pieces if kind != 'stats')
        for end, ref in (('', self.all_ref), ('_stats', self.all_stats_ref)):
            self.wait(ref.at[0], self.sems['pair_recv' + end])
            self.wait(ref.at[0], self.sems['pair_send' + end])
            self.wait(ref.at[0, 0], self.sems['local' + end])
        self.wait(self.all_ref.at[0, others, pl.ds(0, total)], self.sems['plane_send'])
        self.wait(self.all_stats_ref.at[0, others], self.sems['plane_send_stats'])
        self.wait(self.all_ref.at[0, others, pl.ds(0, 3 * self.share_rows)], self.sems['x_send'])


def exchange_kernel(plan, pieces, share_rows, vocab, inv_n, h_ref, own_ref, emb_ref, ids_ref, tgt_ref,
                    all_ref, all_stats_ref, grad_ref, stats_out_ref,
                    logits_ref, m_ref, s_ref, t_ref, col_ref, stats_ref, part_ref, part_recv, part_send, *sem_refs):
    step = pl.program_id(0)
    n_tiles, rows, width = logits_ref.shape
    ex = Exchange(own_ref, stats_ref, all_ref, all_stats_ref, dict(zip(SEMS, sem_refs)), share_rows)

    def run(event):
        kind, *nums = event
        nums = [int(v) for v in nums]
        if kind == 's':
            ex.round(nums[0], pieces[nums[0]], 1)
        elif kind == 'r':
            p, k = nums
            ex.wait_round(p, pieces[p], k)
            if k < 4:
                ex.round(p, pieces[p], k + 1)
            ex.forward(pieces[p], k)
        elif kind == 'x':
            ex.along_x(nums[0])
        else:
            ex.finish_x(nums[0])

    for i, groups in enumerate(plan):
        events = [event for group in groups for event in group.split(',')]
        if events:
            @pl.when(step == i)
            def _(i=i, events=events):
                if i == 0:
                    ex.barrier()
                for event in events:
                    run(event)
                if i == 0:
                    ex.start_own(pieces[0])
                if i == len(plan) - 1:
                    ex.finish(pieces)

    @pl.when(step == 0)
    def _():
        m_ref[...] = jnp.full_like(m_ref, -jnp.inf)
        s_ref[...] = jnp.zeros_like(s_ref)
        t_ref[...] = jnp.zeros_like(t_ref)
        grad_ref[...] = jnp.zeros_like(grad_ref)

    @pl.when(step < n_tiles)
    def _():
        logits = lax.dot_general(h_ref[...], emb_ref[...], NT, preferred_element_type=jnp.float32)
        logits_ref[step] = logits
        lane = lax.broadcasted_iota(jnp.int32, (rows, LANES), 1)
        tgt_sum = t_ref[...]
        parts = []
        for j in range(width // LANES):
            ids = lane + (step * width + j * LANES)
            part = jnp.where(ids < vocab, logits[:, j * LANES:(j + 1) * LANES], -jnp.inf)
            tgt_sum += jnp.where(ids == ids_ref[...], part, 0.0)
            parts.append(part)
        t_ref[...] = tgt_sum
        m_old = m_ref[...]
        m_new = functools.reduce(jnp.maximum, parts, m_old)
        floor = jnp.where(m_new == -jnp.inf, 0.0, m_new)
        s_new = s_ref[...] * jnp.exp(m_old - floor)
        for part in parts:
            s_new += jnp.exp(part - floor)
        m_ref[...] = m_new
        s_ref[...] = s_new

    @pl.when(step == n_tiles)
    def _():
        m_col = jnp.max(m_ref[...], axis=1, keepdims=True)
        s_col = jnp.sum(s_ref[...] * jnp.exp(m_ref[...] - m_col), axis=1, keepdims=True)
        t_col = jnp.sum(t_ref[...], axis=1, keepdims=True)
        lane = lax.broadcasted_iota(jnp.int32, (rows, LANES), 1)
        cols = jnp.where(lane == 0, m_col, jnp.where(lane == 1, s_col, jnp.where(lane == 2, t_col, 0.0)))
        part_ref[ex.x] = cols.T[:8]
        for dx in (1, 2, 3):
            dst = part_ref.at[ex.x]
            pltpu.make_async_remote_copy(
                src_ref=dst, dst_ref=dst, send_sem=part_send, recv_sem=part_recv,
                device_id=ex.at(dx=dx), device_id_type=pl.DeviceIdType.MESH).start()
        ex.wait(part_ref.at[pl.ds(0, 3)], part_recv)
        ex.wait(part_ref.at[pl.ds(0, 3)], part_send)
        m_row = functools.reduce(jnp.maximum, [part_ref[i, 0:1] for i in range(RING)])
        s_row = sum(part_ref[i, 1:2] * jnp.exp(part_ref[i, 0:1] - m_row) for i in range(RING))
        t_row = sum(part_ref[i, 2:3] for i in range(RING))
        sub = lax.broadcasted_iota(jnp.int32, (8, rows), 0)
        values = (m_row, inv_n / s_row, tgt_ref[...], s_row, t_row)
        final = jnp.zeros((8, rows), jnp.float32)
        for i, value in enumerate(values):
            final = jnp.where(sub == i, value, final)
        stats_out_ref[...] = final
        stats_ref[...] = jnp.zeros_like(stats_ref)
        stats_ref[:, :rows] = final
        col_ref[...] = jnp.concatenate([final, jnp.zeros((LANES - 8, rows), jnp.float32)]).T
        ex.start_own(pieces[-1])

    def add_grad(masked):
        tile = step - n_tiles
        ids = lax.broadcasted_iota(jnp.int32, (rows, width), 1) + tile * width
        grad = jnp.exp(logits_ref[tile] - col_ref[:, 0:1]) * col_ref[:, 1:2]
        grad -= jnp.where(ids == ids_ref[...], inv_n, 0.0)
        if masked:
            grad = jnp.where(ids < vocab, grad, 0.0)
        grad = grad.astype(jnp.bfloat16)
        n_cols = grad_ref.shape[1] // 4

        @pl.loop(0, 4)
        def _(j):
            cols = pl.ds(pl.multiple_of(j * n_cols, LANES), n_cols)
            emb = emb_ref[:, cols]
            if masked:
                emb_ids = lax.broadcasted_iota(jnp.int32, emb.shape, 0) + tile * width
                emb = jnp.where(emb_ids < vocab, emb.astype(jnp.float32), 0.0).astype(emb.dtype)
            grad_ref[:, cols] += jnp.dot(grad, emb, preferred_element_type=jnp.float32)

    pl.when(jnp.logical_and(step >= n_tiles, step < 2 * n_tiles - 1))(lambda: add_grad(False))
    pl.when(step == 2 * n_tiles - 1)(lambda: add_grad(True))


def exchange_tokens(h_act, h_wide, emb, local_ids, tgt_row, inv_n, n_dp):
    rows, width = h_act.shape
    vocab = emb.shape[0]
    n_tiles = pl.cdiv(vocab, VOCAB_BLOCK)
    n_steps = 2 * n_tiles + 1
    plan = PLAN if len(PLAN) == n_steps else PLAN[:-1] + ((),) * (n_steps - len(PLAN)) + PLAN[-1:]
    dma = pltpu.SemaphoreType.DMA
    emb_tile = lambda i: (jnp.where(i < n_tiles, i, jnp.minimum(i - n_tiles, n_tiles - 1)), 0)
    whole = pl.BlockSpec(memory_space=pltpu.VMEM)
    return pl.pallas_call(
        functools.partial(exchange_kernel, plan, PIECES, SHARE_ROWS, vocab, inv_n),
        out_shape=(jax.ShapeDtypeStruct((2, n_dp // 2, rows, width), jnp.float32),
                   jax.ShapeDtypeStruct((2, n_dp // 2, 8, 4 * LANES), jnp.float32),
                   jax.ShapeDtypeStruct((rows, width), jnp.float32),
                   jax.ShapeDtypeStruct((8, rows), jnp.float32)),
        grid=(n_steps,),
        in_specs=[whole, whole, pl.BlockSpec((VOCAB_BLOCK, width), emb_tile), whole, whole],
        out_specs=(pl.BlockSpec(memory_space=pl.ANY), pl.BlockSpec(memory_space=pl.ANY), whole, whole),
        scratch_shapes=[pltpu.VMEM((n_tiles, rows, VOCAB_BLOCK), jnp.float32)]
                       + [pltpu.VMEM((rows, LANES), jnp.float32)] * 4
                       + [pltpu.VMEM((8, 4 * LANES), jnp.float32), pltpu.VMEM((RING, 8, rows), jnp.float32)]
                       + [dma, dma, dma((len(PIECES), 4)), dma((4,)), dma((4,))] + [dma] * (len(SEMS) - 3),
        compiler_params=pltpu.CompilerParams(
            vmem_limit_bytes=VMEM_LIMIT, collective_id=0, has_side_effects=True),
        cost_estimate=pl.CostEstimate(
            flops=60 * rows * vocab * width, bytes_accessed=vocab * 4 * width, transcendentals=2 * rows * vocab),
        name="exchange_tokens",
    )(h_act, h_wide, emb, local_ids, tgt_row)


def row_grads(inv_n, emb, row_ids, h_blk, stats, few_rows=False):
    if few_rows:
        logits = lax.dot_general(h_blk, emb, NT, preferred_element_type=jnp.float32).T
    else:
        logits = lax.dot_general(emb, h_blk, NT, preferred_element_type=jnp.float32)
    prob = jnp.exp(logits - stats[0:1]) * stats[1:2]
    grad = prob - jnp.where(row_ids == stats[2:3], inv_n, 0.0)
    return jnp.dot(grad.astype(jnp.bfloat16), h_blk, preferred_element_type=jnp.float32)


def id_column(n_rows, first):
    return (lax.broadcasted_iota(jnp.int32, (n_rows, 1), 0) + first).astype(jnp.float32)


def load_tokens(all_ref, all_stats_ref):
    _, blocks, rows, width = all_ref.shape
    h_blk = all_ref[0].reshape(blocks * rows, width).astype(jnp.bfloat16)
    return h_blk, jnp.concatenate([all_stats_ref[0, i, :, :rows] for i in range(blocks)], axis=1)


def token_specs(gathered, pos_block):
    return [pl.BlockSpec((1, pos_block) + arr.shape[2:],
                         lambda i, where: (i * pos_block // arr.shape[1], lax.rem(i, arr.shape[1] // pos_block), 0, 0))
            for arr in gathered]


def own_rows_kernel(inv_n, bases, where, emb0_ref, emb1_ref, all_ref, all_stats_ref, own0_ref, own1_ref,
                    emb_ref, acc_ref, stage_ref, sem):
    n0, n1 = emb0_ref.shape[0], emb1_ref.shape[0]
    step, n_steps = pl.program_id(0), pl.num_programs(0)
    depth, n_pos = stage_ref.shape[0], stage_ref.shape[1]
    per_core = all_ref.shape[1] // n_pos

    def load(i):
        src = all_ref.at[i // per_core, pl.ds(lax.rem(i, per_core) * n_pos, n_pos)]
        slot = lax.rem(i, depth)
        return pltpu.make_async_copy(src, stage_ref.at[slot], sem.at[slot])

    @pl.when(step == 0)
    def _():
        for i in range(depth - 1):
            load(i).start()

    load(step).wait()

    @pl.when(step + depth - 1 < n_steps)
    def _():
        load(step + depth - 1).start()


    @pl.when(pl.program_id(0) == 0)
    def _():
        emb_ref[:n0] = emb0_ref[...]
        emb_ref[n0:] = emb1_ref[...]
        acc_ref[...] = jnp.zeros_like(acc_ref)

    first0, first1 = [where[1] + base + where[0] * n for base, n in zip(bases, (n0, n1))]
    row = lax.broadcasted_iota(jnp.int32, (n0 + n1, 1), 0)
    row_ids = (row + jnp.where(row < n0, first0, first1 - n0)).astype(jnp.float32)
    h_blk, stats = load_tokens(stage_ref.at[pl.ds(lax.rem(step, depth), 1)], all_stats_ref)
    acc_ref[...] += row_grads(inv_n, emb_ref[...], row_ids, h_blk, stats, True)

    @pl.when(pl.program_id(0) == pl.num_programs(0) - 1)
    def _():
        own0_ref[...] = acc_ref[:n0]
        own1_ref[:n1] = acc_ref[n0:]
        own1_ref[n1:] = jnp.zeros_like(own1_ref[n1:])


def own_rows(emb, gathered, where, inv_n, n_dp):
    width = emb.shape[1]
    n_tok = gathered[0].size // width
    n0, n1 = GRAD_CHUNKS
    bases = (0, n_dp * n0)
    emb_spec = lambda base, n: pl.BlockSpec((n, width), lambda i, where: (base // n + where[0], 0))
    whole = lambda n: pl.BlockSpec((n, width), lambda i, where: (0, 0))
    return pl.pallas_call(
        functools.partial(own_rows_kernel, inv_n, bases),
        out_shape=(jax.ShapeDtypeStruct((n0, width), jnp.float32), jax.ShapeDtypeStruct((n1 + 8, width), jnp.float32)),
        grid_spec=pltpu.PrefetchScalarGridSpec(
            num_scalar_prefetch=1,
            grid=(gathered[0].shape[0] * gathered[0].shape[1] // OWN_POS_BLOCK,),
            in_specs=[emb_spec(bases[0], n0), emb_spec(bases[1], n1),
                      pl.BlockSpec(memory_space=pl.ANY), token_specs(gathered, OWN_POS_BLOCK)[1]],
            out_specs=(whole(n0), whole(n1 + 8)),
            scratch_shapes=[pltpu.VMEM((n0 + n1, width), jnp.bfloat16), pltpu.VMEM((n0 + n1, width), jnp.float32),
                            pltpu.VMEM((OWN_DEPTH, OWN_POS_BLOCK) + gathered[0].shape[2:], jnp.float32),
                            pltpu.SemaphoreType.DMA((OWN_DEPTH,))]),
        compiler_params=pltpu.CompilerParams(vmem_limit_bytes=VMEM_LIMIT),
        cost_estimate=pl.CostEstimate(
            flops=4 * (n0 + n1) * n_tok * width, bytes_accessed=n_tok * width * 4, transcendentals=(n0 + n1) * n_tok),
        name="own_rows",
    )(where, emb, emb, *gathered)


def first_block_kernel(inv_n, first, where, emb_ref, all_ref, all_stats_ref, out_ref, copy_ref, h_ref, stats_ref):
    step, last = pl.program_id(0), pl.num_programs(0) - 1

    @pl.when(step == 0)
    def _():
        out_ref[...] = jnp.zeros_like(out_ref)

    h_blk, stats = load_tokens(all_ref, all_stats_ref)
    h_ref[...] = h_blk
    stats_ref[...] = stats
    n_rows = emb_ref.shape[0]
    row_ids = id_column(n_rows, where[1] + where[2] * ROW_BLOCK + first)
    out_ref[...] += row_grads(inv_n, emb_ref[...], row_ids, h_blk, stats)

    @pl.when(step == last)
    def _():
        copy_ref[...] = out_ref[...]


def first_block(emb, gathered, where, inv_n, first, n_blocks):
    vocab, width = emb.shape
    n_tok = gathered[0].size // width
    per_step = POS_BLOCK * gathered[0].shape[2]
    rows = n_blocks * ROW_BLOCK
    row_spec = pl.BlockSpec((rows, width), lambda i, where: ((first + where[2]) // n_blocks, 0), pipeline_mode=pl.Buffered(1))
    return pl.pallas_call(
        functools.partial(first_block_kernel, inv_n, first * ROW_BLOCK),
        out_shape=(jax.ShapeDtypeStruct((vocab, width), jnp.float32),
                   jax.ShapeDtypeStruct((rows, width), jnp.float32),
                   jax.ShapeDtypeStruct((n_tok, width), jnp.bfloat16),
                   jax.ShapeDtypeStruct((8, n_tok), jnp.float32)),
        grid_spec=pltpu.PrefetchScalarGridSpec(
            num_scalar_prefetch=1,
            grid=(n_tok // per_step,),
            in_specs=[row_spec] + token_specs(gathered, POS_BLOCK),
            out_specs=(row_spec, pl.BlockSpec((rows, width), lambda i, where: (0, 0), pipeline_mode=pl.Buffered(1)),
                       pl.BlockSpec((per_step, width), lambda i, where: (i, 0)),
                       pl.BlockSpec((8, per_step), lambda i, where: (0, i)))),
        compiler_params=pltpu.CompilerParams(vmem_limit_bytes=VMEM_LIMIT),
        cost_estimate=pl.CostEstimate(
            flops=4 * rows * n_tok * width, bytes_accessed=n_tok * width * 6, transcendentals=rows * n_tok),
        name="first_block",
    )(where, emb, *gathered)


class Placing:
    def __init__(self, out_ref, got_ref, recv_refs, recv_rows, n_steps, stages, sems):
        self.out_ref, self.got_ref, self.recv_refs, self.recv_rows = out_ref, got_ref, recv_refs, recv_rows
        self.n_steps, self.stages, self.sems = n_steps, stages, sems
        self.per_step = got_ref.shape[0] // n_steps
        self.n_got = stages[0].shape[2]
        self.n_recv = stages[1].shape[1]
        self.parts = recv_refs[0].shape[0] // self.n_recv

    def copies(self, step, slot, store):
        sem = self.sems.at[1 if store else 0, slot]
        for j in range(self.per_step):
            i = step * self.per_step + j
            stage = self.stages[0].at[slot, j]
            if store:
                yield pltpu.make_async_copy(stage, self.out_ref.at[pl.ds(pl.multiple_of(i * self.n_got, 8), self.n_got)], sem)
            else:
                yield pltpu.make_async_copy(self.got_ref.at[i, pl.ds(0, self.n_got)], stage, sem)

    def recv_copy(self, step, slot, store, k):
        sem = self.sems.at[3 if store else 2, slot]
        part = (step - k * self.parts) * self.n_recv
        stage = self.stages[1].at[slot]
        if store:
            row = pl.multiple_of(self.recv_rows[k] + part, 8)
            return pltpu.make_async_copy(stage, self.out_ref.at[pl.ds(row, self.n_recv)], sem)
        return pltpu.make_async_copy(self.recv_refs[k].at[pl.ds(pl.multiple_of(part, 8), self.n_recv)], stage, sem)

    def each(self, step, store, act):
        slot = lax.rem(step, 2)
        for copy in self.copies(step, slot, store):
            act(copy)
        for k in range(len(self.recv_refs)):
            @pl.when(jnp.logical_and(step >= k * self.parts, step < (k + 1) * self.parts))
            def _(k=k):
                act(self.recv_copy(step, slot, store, k))

    def before(self, step):
        @pl.when(step >= 1)
        def _():
            self.each(step - 1, False, lambda c: c.wait())
            self.each(step - 1, True, lambda c: c.start())

        @pl.when(step >= 2)
        def _():
            self.each(step - 2, True, lambda c: c.wait())

        self.each(step, False, lambda c: c.start())

    def after(self, step):
        @pl.when(step == self.n_steps - 1)
        def _():
            self.each(step, False, lambda c: c.wait())
            self.each(step, True, lambda c: c.start())
            self.each(step - 1, True, lambda c: c.wait())
            self.each(step, True, lambda c: c.wait())


def grad_rows_kernel(inv_n, first, n_steps, recv_firsts, where, emb_ref, h_ref, stats_ref, *refs):
    step = pl.program_id(0)
    n_ref = 2 + len(recv_firsts) if recv_firsts else 1
    out_in_ref, acc_ref, copy_ref = refs[0], refs[n_ref], refs[n_ref + 1]
    n_rows = emb_ref.shape[0]
    placing = None
    if recv_firsts:
        rows = [(where[3] + block) * n_rows for block in recv_firsts]
        placing = Placing(out_in_ref, refs[1], refs[2:n_ref], rows, n_steps, refs[n_ref + 2:n_ref + 4], refs[n_ref + 4])
        placing.before(step)

    @pl.when(step == 0)
    def _():
        acc_ref[...] = jnp.zeros_like(acc_ref)

    row_ids = id_column(n_rows, where[1] + (where[2] + first) * n_rows)
    acc_ref[...] += row_grads(inv_n, emb_ref[...], row_ids, h_ref[...], stats_ref[...])

    @pl.when(step == pl.num_programs(0) - 1)
    def _():
        copy_ref[...] = acc_ref[...]

    if placing:
        placing.after(step)


def grad_rows(emb, h_all, stats, where, out, inv_n, first, got=None, n_got=0, recvs=(), recv_firsts=()):
    vocab, width = emb.shape
    n_tok = h_all.shape[0]
    tok_block = min(TOKEN_BLOCK, n_tok)
    n_steps = n_tok // tok_block
    row_spec = pl.BlockSpec((ROW_BLOCK, width), lambda t, where: (first + where[2], 0), pipeline_mode=pl.Buffered(1))
    anywhere = pl.BlockSpec(memory_space=pl.ANY)
    in_specs = [row_spec, pl.BlockSpec((tok_block, width), lambda t, where: (t, 0)),
                pl.BlockSpec((8, tok_block), lambda t, where: (0, t)), anywhere]
    args, scratch = [emb, h_all, stats, out], []
    if recvs:
        args += [got, *recvs]
        in_specs += [anywhere] * (1 + len(recvs))
        n_recv = recvs[0].shape[0]
        part = n_recv * len(recvs) // n_steps
        part = next(n for n in range(part // 8 * 8 or 8, n_recv + 1, 8) if n_recv % n == 0 and n * n_steps >= n_recv * len(recvs))
        scratch = [pltpu.VMEM((2, got.shape[0] // n_steps, n_got, width), jnp.float32),
                   pltpu.VMEM((2, part, width), jnp.float32), pltpu.SemaphoreType.DMA((4, 2))]
    return pl.pallas_call(
        functools.partial(grad_rows_kernel, inv_n, first, n_steps, tuple(recv_firsts)),
        out_shape=(jax.ShapeDtypeStruct((vocab, width), jnp.float32), jax.ShapeDtypeStruct((ROW_BLOCK, width), jnp.float32)),
        grid_spec=pltpu.PrefetchScalarGridSpec(
            num_scalar_prefetch=1,
            grid=(n_steps,),
            in_specs=in_specs,
            out_specs=(row_spec, pl.BlockSpec((ROW_BLOCK, width), lambda t, where: (0, 0), pipeline_mode=pl.Buffered(1))),
            scratch_shapes=scratch),
        input_output_aliases={4: 0},
        compiler_params=pltpu.CompilerParams(vmem_limit_bytes=VMEM_LIMIT),
        cost_estimate=pl.CostEstimate(
            flops=4 * ROW_BLOCK * n_tok * width, bytes_accessed=n_tok * width * 2, transcendentals=ROW_BLOCK * n_tok),
        name="grad_rows",
    )(where, *args)


def place_kernel(where, src_ref, prev_ref, dst_ref, *sum_refs):
    del where, prev_ref
    n_dev, n_rows = src_ref.shape[0], dst_ref.shape[0] // src_ref.shape[0]
    for i in range(n_dev):
        dst_ref[i * n_rows:(i + 1) * n_rows] = src_ref[i, :n_rows]
    for sum_ref in sum_refs:
        @pl.when(pl.program_id(0) == 0)
        def _(sum_ref=sum_ref):
            sum_ref[...] = jnp.zeros_like(sum_ref)

        sum_ref[...] += sum(src_ref[i, n_rows:] for i in range(n_dev))


def place_rows(src, n_rows, out, where, first_block, per_block, with_sums=False):
    n_src, n_in, width = src.shape
    placed = pl.pallas_call(
        place_kernel,
        out_shape=[jax.ShapeDtypeStruct(out.shape, out.dtype)]
                  + [jax.ShapeDtypeStruct((n_in - n_rows, width), out.dtype)] * with_sums,
        grid_spec=pltpu.PrefetchScalarGridSpec(
            num_scalar_prefetch=1,
            grid=(n_src // per_block,),
            in_specs=[pl.BlockSpec((per_block, n_in, width), lambda i, where: (i, 0, 0)),
                      pl.BlockSpec(memory_space=pl.ANY)],
            out_specs=[pl.BlockSpec((per_block * n_rows, width), lambda i, where: (i + first_block + where[3], 0))]
                      + [pl.BlockSpec((n_in - n_rows, width), lambda i, where: (0, 0))] * with_sums),
        input_output_aliases={2: 0},
        compiler_params=pltpu.CompilerParams(vmem_limit_bytes=VMEM_LIMIT),
        cost_estimate=pl.CostEstimate(flops=src.size * 80, bytes_accessed=src.size * 8, transcendentals=0),
        name="place_rows",
    )(where, src, out)
    return placed if with_sums else placed[0]


def shifts(n_tp):
    return [[(i, (i + shift) % n_tp) for i in range(n_tp)] for shift in range(1, n_tp)]


def send_blocks(part, n_tp, tp_idx):
    blocks = part.reshape(n_tp, part.shape[0] // n_tp, part.shape[1])
    pick = lambda i: lax.dynamic_index_in_dim(blocks, i % n_tp, 0, keepdims=False)
    return [pick(tp_idx)] + [lax.ppermute(pick(tp_idx + 1 + d), 'tp', perm) for d, perm in enumerate(shifts(n_tp))]


def send_total(blocks, n_tp):
    total = functools.reduce(jnp.add, blocks)
    return [total] + [lax.ppermute(total, 'tp', perm) for perm in shifts(n_tp)]


def join_totals(totals, n_tp, tp_idx):
    whole = jnp.zeros((n_tp,) + totals[0].shape, totals[0].dtype)
    for shift, total in enumerate(totals):
        whole = lax.dynamic_update_index_in_dim(whole, total, (tp_idx + n_tp - shift) % n_tp, 0)
    return whole.reshape(-1, totals[0].shape[1])


def solution(mesh):
    n_tp, n_dp = mesh.shape['tp'], mesh.shape['dp']

    def program(hidden, residual, targets, embedding, norm_w):
        inv_n = 1.0 / (hidden.shape[0] * hidden.shape[1])

        def local_part(hid_loc, res_loc, tgt_loc, emb_loc, norm_vec):
            n_batch, n_seq, d_model = hid_loc.shape
            n_rows = n_batch * n_seq
            vocab_loc = emb_loc.shape[0]
            tp_idx, dp_idx = lax.axis_index('tp'), lax.axis_index('dp')
            resid = (res_loc + hid_loc.astype(jnp.float32)).reshape(n_rows, d_model)
            tgt_rows = tgt_loc.reshape(n_rows)
            inv_rms = lax.rsqrt(jnp.mean(resid * resid, axis=-1, keepdims=True) + NORM_EPS)
            scaled_r = resid * inv_rms
            h_wide = lax.reduce_precision(scaled_r * norm_vec, exponent_bits=8, mantissa_bits=7)
            h_act = h_wide.astype(jnp.bfloat16)
            local_ids = (tgt_rows - tp_idx * vocab_loc)[:, None]
            local_ids = jnp.where(local_ids < vocab_loc, local_ids, -1)
            tgt_row = tgt_rows.astype(jnp.float32)[None]
            *gathered, grad_h, stats = exchange_tokens(h_act, h_wide, emb_loc, local_ids, tgt_row, inv_n, n_dp)
            loss_part = jnp.sum(stats[0] + jnp.log(stats[3]) - stats[4]) * inv_n

            per_core = sum(BLOCK_CALLS)
            core = dp_idx % 2
            where = jnp.stack([dp_idx, tp_idx * vocab_loc, core * per_core, (1 - core) * per_core]).astype(jnp.int32)
            own0, own1 = own_rows(emb_loc, gathered, where, inv_n, n_dp)
            got0 = lax.all_gather(own0, 'dp')
            gathered, grad_h, own0 = lax.optimization_barrier((gathered, grad_h, own0))
            grad_h = send_blocks(grad_h, n_tp, tp_idx)

            first = n_dp * sum(GRAD_CHUNKS) // ROW_BLOCK
            pair = [(i, i ^ 1) for i in range(n_dp)]
            out, copied, h_all, all_stats = first_block(emb_loc, gathered, where, inv_n, first, BLOCK_CALLS[0])
            recvs, recv_firsts, late, block = [], [], [], first
            for c, n_blocks in enumerate(BLOCK_CALLS):
                final = c == len(BLOCK_CALLS) - 1
                if c:
                    extra = (got0, GRAD_CHUNKS[0], recvs, recv_firsts) if final else ()
                    out, copied = grad_rows(emb_loc, h_all, all_stats, where, out, inv_n, block, *extra)
                if c < 2:
                    grad_h, out = lax.optimization_barrier((grad_h, out))
                    grad_h = join_totals(grad_h, n_tp, tp_idx) if c else send_total(grad_h, n_tp)
                recv = lax.ppermute(copied, 'dp', pair)
                if c < len(BLOCK_CALLS) - 2:
                    recvs.append(recv)
                    recv_firsts.append(block)
                else:
                    late.append((recv, block))
                block += n_blocks
                if c == 1:
                    grad_scaled = grad_h * norm_vec
                    grad_r = inv_rms * (grad_scaled - scaled_r * jnp.mean(grad_scaled * scaled_r, axis=-1, keepdims=True))
                    grad_w = jnp.sum(grad_h * scaled_r, axis=0)
                    own1 = own1.at[-8].set(grad_w).at[-7, 0].set(loss_part)
                    got1 = lax.all_gather(own1, 'dp')

            n_own = GRAD_CHUNKS[1]
            n_place = PLACE_BLOCK * n_own
            (recv, block), (last_recv, last_block) = late
            for part, start in ((recv, block), (last_recv, last_block)):
                out = place_rows(part.reshape(-1, ROW_BLOCK, d_model), ROW_BLOCK, out, where, start, 1)
            out, sums = place_rows(got1, n_own, out, jnp.zeros_like(where), n_dp * GRAD_CHUNKS[0] // n_place, PLACE_BLOCK, True)
            return sums[1, 0], grad_r.reshape(n_batch, n_seq, d_model), out, sums[0]

        sharded = jax.shard_map(
            local_part, mesh=mesh,
            in_specs=(P('dp', None, None), P('dp', None, None), P('dp', None), P('tp', None), P(None)),
            out_specs=(P(), P('dp', None, None), P('tp', None), P(None)),
            check_vma=False)
        return sharded(hidden, residual, targets, embedding, norm_w)

    return program
```
